32 devices in a mesh: gx: 4 (over y, core), gy: 8 (over z, x).
Axes of the slice: x: 2, y: 2, z: 4, core: 2. Of those that a mesh axis runs over, the one named last changes fastest.
Arguments:
- conserved: float32 [5, 16, 128, 128], P(None, 'gx', 'gy'), as said below
Outputs:
- increment: float32 [5, 16, 128, 128], P(None, 'gx', 'gy')
- blending: float32 [4, 32, 32], P('gx', 'gy')
Inputs may be any that keep to these rules, and one draw needn't show every extreme that they name: `conserved`: every node's density and pressure are positive.
All inputs are finite; a program needn't handle non-finite values. Where the reference program divides by a largest or mean magnitude, that divisor is 1e-20 or more.
Results may differ from the reference program's by a relative error of at most 0.0003.
Values sent between devices are 32-bit elements; how exact they have to be, the bound alone decides.
A program may use at most 64 MiB of HBM per device.

```python
import math
import jax
import jax.numpy as jnp
import numpy as np
from jax import lax

EZ = 32
EX = 4
EY = 32


def log_uniform(subkey, lower, upper, layout):
    return jnp.exp(jax.random.uniform(subkey, layout, jnp.float32, math.log(lower), math.log(upper)))


def draw_conserved(key, part):
    subkeys = jax.random.split(key, 7)
    element_shape = (EX, 1, EY, 1, EZ, 1)
    node_shape = (EX, 4, EY, 4, EZ, 4)
    inverse_root = 1.0 / math.sqrt(5.0)
    points = jnp.array([-1.0, -inverse_root, inverse_root, 1.0], jnp.float32)
    coord_x = points.reshape(1, 4, 1, 1, 1, 1)
    coord_y = points.reshape(1, 1, 1, 4, 1, 1)
    coord_z = points.reshape(1, 1, 1, 1, 1, 4)
    index_x = jnp.arange(EX, dtype=jnp.int32).reshape(EX, 1, 1, 1, 1, 1)
    index_y = jnp.arange(EY, dtype=jnp.int32).reshape(1, 1, EY, 1, 1, 1)
    index_z = jnp.arange(EZ, dtype=jnp.int32).reshape(1, 1, 1, 1, EZ, 1)
    rough = (2 * index_x + index_y + 3 * index_z) % 8 == 0
    amplitude = jnp.where(rough, log_uniform(subkeys[0], 0.1, 0.2, element_shape), 0.0)
    base_density = log_uniform(subkeys[1], 0.5, 2.0, element_shape)
    base_pressure = log_uniform(subkeys[2], 0.5, 2.0, element_shape)
    base_velocity = 0.3 * jax.random.normal(subkeys[3], (3,) + element_shape, jnp.float32)
    density_slopes = jax.random.uniform(subkeys[5], (3,) + element_shape, jnp.float32, -1.0, 1.0)
    velocity_slopes = jax.random.uniform(subkeys[6], (3, 3) + element_shape, jnp.float32, -1.0, 1.0)
    jitter = jnp.clip(jax.random.normal(subkeys[4], (5,) + node_shape, jnp.float32), -4.0, 4.0)
    linear_density = 1.0 + 0.3 * (density_slopes[0] * coord_x + density_slopes[1] * coord_y + density_slopes[2] * coord_z)
    linear_velocity = 0.6 * (velocity_slopes[:, 0] * coord_x + velocity_slopes[:, 1] * coord_y + velocity_slopes[:, 2] * coord_z)
    layout = (4 * EX, 4 * EY, 4 * EZ)
    density = (base_density * linear_density * jnp.exp(amplitude * jitter[0])).reshape(layout)
    pressure = jnp.broadcast_to(base_pressure * jnp.exp(amplitude * jitter[1]), node_shape).reshape(layout)
    velocity = (base_velocity + linear_velocity + amplitude * jitter[2:5]).reshape((3,) + layout)
    energy = pressure / 0.4 + 0.5 * density * jnp.sum(velocity * velocity, axis=0)
    return jnp.stack([density, density * velocity[0], density * velocity[1], density * velocity[2], energy]).astype(jnp.float32)


def setup_inputs(seed: int = 0) -> dict:
    key_of = jax.random.split(jax.random.key(seed), 2)
    return {
        "conserved": draw_conserved(jax.random.fold_in(key_of[1], 71), 0),
    }


gas_gamma = 1.4

def tables():
    inverse_root = 1.0 / math.sqrt(5.0)
    points = np.array([-1.0, -inverse_root, inverse_root, 1.0])
    weights = [1.0 / 6.0, 5.0 / 6.0, 5.0 / 6.0, 1.0 / 6.0]
    barycentric = np.array([1.0 / np.prod([points[target] - points[other] for other in range(4) if other != target]) for target in range(4)])
    derivative = np.zeros((4, 4))
    for target in range(4):
        for source in range(4):
            if target != source:
                derivative[target, source] = barycentric[source] / barycentric[target] / (points[target] - points[source])
    legendre = np.stack([np.ones(4), points, (3.0 * points ** 2 - 1.0) / 2.0, (5.0 * points ** 3 - 3.0 * points) / 2.0], 1)
    legendre = legendre * np.sqrt(np.arange(4) + 0.5)
    weight_column = np.array(weights)[:, None]
    discrete_norms = np.sum(weight_column * legendre * legendre, 0)
    inverse = (weight_column * legendre).T / discrete_norms[:, None]
    return (weights, derivative, inverse)

def describe(conserved):
    density = conserved[0]
    velocity = conserved[1:4] / density
    pressure = (gas_gamma - 1.0) * (conserved[4] - 0.5 * density * lax.optimization_barrier(jnp.sum(velocity * velocity, axis=0)))
    sound_speed = jnp.sqrt(gas_gamma * pressure / density)
    return (conserved, density, velocity, pressure, sound_speed)

def log_mean(left_value, right_value):
    relative = (left_value - right_value) / (left_value + right_value)
    square = relative * relative
    series = 1.0 + square / 3.0 + square * square / 5.0 + square * square * square / 7.0
    safe_relative = jnp.where(square < 0.01, 1.0, relative)
    logarithmic = jnp.log(left_value / right_value) / (2.0 * safe_relative)
    factor = jnp.where(square < 0.01, series, logarithmic)
    return (left_value + right_value) / (2.0 * factor)

def entropy_flux(left_state, right_state, normal):
    left_density, left_velocity, left_pressure = (left_state[1], left_state[2], left_state[3])
    right_density, right_velocity, right_pressure = (right_state[1], right_state[2], right_state[3])
    mean_density = log_mean(left_density, right_density)
    inverse_beta = 1.0 / log_mean(left_density / left_pressure, right_density / right_pressure)
    mean_velocity = 0.5 * (left_velocity + right_velocity)
    mean_pressure = 0.5 * (left_pressure + right_pressure)
    square_mean = 0.5 * lax.optimization_barrier(jnp.sum(left_velocity * right_velocity, axis=0))
    mass_flux = mean_density * mean_velocity[normal]
    components = [mass_flux]
    for other in range(3):
        momentum = mass_flux * mean_velocity[other]
        if other == normal:
            momentum = momentum + mean_pressure
        components.append(momentum)
    energy_flux = mass_flux * (square_mean + inverse_beta / (gas_gamma - 1.0)) + 0.5 * (left_pressure * right_velocity[normal] + right_pressure * left_velocity[normal])
    components.append(energy_flux)
    return jnp.stack(components)

def surface_flux(left_state, right_state, normal):
    largest = jnp.maximum(jnp.abs(left_state[2][normal]) + left_state[4], jnp.abs(right_state[2][normal]) + right_state[4])
    return entropy_flux(left_state, right_state, normal) - 0.5 * largest * (right_state[0] - left_state[0])

def accumulate(total, term):
    return term if total is None else total + term

def direction_terms(padded, dimension):
    weights, derivative, inverse = tables()
    elements = (padded.shape[dimension] - 2) // 4

    def nodes_from(start):
        return describe(lax.slice_in_dim(padded, start, start + 4 * (elements - 1) + 1, 4, dimension))
    node_states = [nodes_from(1 + position) for position in range(4)]
    previous = nodes_from(0)
    following = nodes_from(5)
    normal = dimension - 1
    high_order = [None, None, None, None]
    for first in range(4):
        for second in range(first + 1, 4):
            pair_flux = entropy_flux(node_states[first], node_states[second], normal)
            high_order[first] = accumulate(high_order[first], 2.0 * float(derivative[first, second]) * pair_flux)
            high_order[second] = accumulate(high_order[second], 2.0 * float(derivative[second, first]) * pair_flux)
    lower_face = surface_flux(previous, node_states[0], normal)
    upper_face = surface_flux(node_states[3], following, normal)
    high_order[0] = high_order[0] - lower_face / weights[0]
    high_order[3] = high_order[3] + upper_face / weights[3]
    face_flux = [lower_face] + [surface_flux(node_states[position], node_states[position + 1], normal) for position in range(3)] + [upper_face]
    subcell = [(face_flux[position + 1] - face_flux[position]) / weights[position] for position in range(4)]
    layout = list(padded.shape)
    layout[dimension] = 4 * elements
    return (jnp.stack(high_order, dimension + 1).reshape(layout), jnp.stack(subcell, dimension + 1).reshape(layout))

def tendency(padded, blend_weights):
    along_x = padded[:, :, 1:-1]
    along_y = padded[:, 1:-1]
    center = padded[:, 1:-1, 1:-1]
    along_z = jnp.concatenate([center[..., -1:], center, center[..., :1]], axis=3)
    high_x, subcell_x = direction_terms(along_x, 1)
    high_y, subcell_y = direction_terms(along_y, 2)
    high_z, subcell_z = direction_terms(along_z, 3)
    high_total = high_x + high_y + high_z
    subcell_total = subcell_x + subcell_y + subcell_z
    return -((1.0 - blend_weights) * high_total + blend_weights * subcell_total)

def indicator(conserved):
    weights, derivative, inverse = tables()
    state = describe(conserved)
    indicated = state[1] * state[3]
    extent = indicated.shape
    grouped = indicated.reshape(extent[0] // 4, 4, extent[1] // 4, 4, extent[2] // 4, 4)
    matrix = jnp.asarray(inverse, jnp.float32)
    coefficients = jnp.einsum('ai,bj,ck,xiyjzk->abcxyz', matrix, matrix, matrix, grouped, precision=lax.Precision.HIGHEST)
    squares = coefficients * coefficients
    energy_all = lax.optimization_barrier(jnp.sum(squares, axis=(0, 1, 2)))
    energy_three = lax.optimization_barrier(jnp.sum(squares[:3, :3, :3], axis=(0, 1, 2)))
    energy_two = lax.optimization_barrier(jnp.sum(squares[:2, :2, :2], axis=(0, 1, 2)))
    energy = jnp.maximum((energy_all - energy_three) / (energy_all + 1e-06), (energy_three - energy_two) / (energy_three + 1e-06))
    threshold = 0.5 * 10.0 ** (-1.8 * 4.0 ** 0.25)
    sharpness = math.log(9999.0)
    raw_blend = 1.0 / (1.0 + jnp.exp(-(sharpness / threshold) * (energy - threshold)))
    return jnp.minimum(raw_blend, 0.5)

def smooth(raw_blend, x_lower, x_upper, y_lower, y_upper):
    extended_x = jnp.concatenate([x_lower, raw_blend, x_upper], axis=0)
    extended_y = jnp.concatenate([y_lower, raw_blend, y_upper], axis=1)
    neighbours = jnp.maximum(extended_x[:-2], extended_x[2:])
    neighbours = jnp.maximum(neighbours, jnp.maximum(extended_y[:, :-2], extended_y[:, 2:]))
    neighbours = jnp.maximum(neighbours, jnp.maximum(jnp.roll(raw_blend, 1, 2), jnp.roll(raw_blend, -1, 2)))
    return jnp.maximum(raw_blend, 0.5 * neighbours)

def blend_nodes(blending):
    extent = blending.shape
    spread = jnp.broadcast_to(blending[:, None, :, None, :, None], (extent[0], 4, extent[1], 4, extent[2], 4))
    return spread.reshape(4 * extent[0], 4 * extent[1], 4 * extent[2])

def reference(conserved):
    state = describe(conserved)
    top_speed = jnp.max(lax.optimization_barrier(jnp.sum(jnp.abs(state[2]), axis=0)) + 3.0 * state[4])
    time_step = 0.25 / top_speed
    raw_blend = indicator(conserved)
    blending = smooth(raw_blend, raw_blend[-1:], raw_blend[:1], raw_blend[:, -1:], raw_blend[:, :1])
    blend_full = blend_nodes(blending)
    nodes_x = conserved.shape[1]

    def column(column_index):
        positions = (4 * column_index - 1 + jnp.arange(6, dtype=jnp.int32)) % nodes_x
        slab_state = jnp.take(conserved, positions.astype(jnp.int32), axis=1)
        slab_state = jnp.concatenate([slab_state[:, :, -1:], slab_state, slab_state[:, :, :1]], axis=2)
        slab_blend = lax.dynamic_slice_in_dim(blend_full, (4 * column_index).astype(jnp.int32), 4, 0)
        return time_step * tendency(slab_state, slab_blend)
    columns = lax.map(column, jnp.arange(nodes_x // 4, dtype=jnp.int32))
    increment = jnp.transpose(columns, (1, 0, 2, 3, 4)).reshape(conserved.shape)
    return (increment, blending)
```

```python
import math

import jax
import jax.numpy as jnp
import numpy as np
from jax import lax
from jax.experimental import pallas as pl
from jax.experimental.pallas import tpu as pltpu
from jax.sharding import PartitionSpec as P

gas_gamma = 1.4
MESH = pl.DeviceIdType.MESH
BASE = 8
VEL, PRS, SND, LND, LNR, RAT = 5, 8, 9, 10, 11, 12
FIELDS = 13


def tables():
    inverse_root = 1.0 / math.sqrt(5.0)
    points = np.array([-1.0, -inverse_root, inverse_root, 1.0])
    weights = [1.0 / 6.0, 5.0 / 6.0, 5.0 / 6.0, 1.0 / 6.0]
    barycentric = np.array(
        [
            1.0 / np.prod([points[target] - points[other] for other in range(4) if other != target])
            for target in range(4)
        ]
    )
    derivative = np.zeros((4, 4))
    for target in range(4):
        for source in range(4):
            if target != source:
                derivative[target, source] = (
                    barycentric[source] / barycentric[target] / (points[target] - points[source])
                )
    legendre = np.stack(
        [np.ones(4), points, (3.0 * points**2 - 1.0) / 2.0, (5.0 * points**3 - 3.0 * points) / 2.0],
        1,
    )
    legendre = legendre * np.sqrt(np.arange(4) + 0.5)
    weight_column = np.array(weights)[:, None]
    discrete_norms = np.sum(weight_column * legendre * legendre, 0)
    inverse = (weight_column * legendre).T / discrete_norms[:, None]
    return (weights, derivative, inverse)


def mechanics(conserved):
    density, m1, m2, m3, energy = conserved
    inverse = 1.0 / density
    v1, v2, v3 = m1 * inverse, m2 * inverse, m3 * inverse
    pressure = (gas_gamma - 1.0) * (energy - 0.5 * density * (v1 * v1 + v2 * v2 + v3 * v3))
    sound = jnp.sqrt(gas_gamma * pressure * inverse)
    return [v1, v2, v3, pressure, sound]


def logarithms(density, pressure):
    ratio = density / pressure
    return [jnp.log(density), jnp.log(ratio), ratio]


def primitives(conserved):
    motion = mechanics(conserved)
    return list(conserved) + motion + logarithms(conserved[0], motion[3])


def mean_parts(a, b, log_a, log_b):
    total, gap = a + b, a - b
    relative = gap / total
    square = relative * relative
    small = square < 0.01
    series = 2.0 + square * (2.0 / 3.0 + square * (2.0 / 5.0 + square * (2.0 / 7.0)))
    return jnp.where(small, total, gap), jnp.where(small, series, log_a - log_b)


def entropy_flux(a, b, normal):
    num, den = mean_parts(a[0], b[0], a[LND], b[LND])
    mean_density = num / den
    num, den = mean_parts(a[RAT], b[RAT], a[LNR], b[LNR])
    inverse_beta = den / num
    velocity = [0.5 * (a[VEL + i] + b[VEL + i]) for i in range(3)]
    pressure = 0.5 * (a[PRS] + b[PRS])
    product = 0.5 * (a[5] * b[5] + a[6] * b[6] + a[7] * b[7])
    mass = mean_density * velocity[normal]
    out = [mass]
    for other in range(3):
        momentum = mass * velocity[other]
        out.append(momentum + pressure if other == normal else momentum)
    out.append(
        mass * (product + inverse_beta * (1.0 / (gas_gamma - 1.0)))
        + 0.5 * (a[PRS] * b[VEL + normal] + b[PRS] * a[VEL + normal])
    )
    return out


def dissipated(flux, a, b, normal):
    half = 0.5 * jnp.maximum(
        jnp.abs(a[VEL + normal]) + a[SND], jnp.abs(b[VEL + normal]) + b[SND]
    )
    return [flux[i] - half * (b[i] - a[i]) for i in range(5)]


def line_terms(nodes, normal, weights, deriv):
    vol = [[0.0] * 5 for _ in range(4)]
    diff = [[0.0] * 5 for _ in range(4)]
    for i in range(4):
        for j in range(i + 1, 4):
            flux = entropy_flux(nodes[i], nodes[j], normal)
            ci, cj = 2.0 * float(deriv[i, j]), 2.0 * float(deriv[j, i])
            if j == i + 1:
                face = dissipated(flux, nodes[i], nodes[j], normal)
            for f in range(5):
                vi, vj = ci * flux[f], cj * flux[f]
                vol[i][f] = vol[i][f] + vi
                vol[j][f] = vol[j][f] + vj
                if j == i + 1:
                    diff[i][f] = diff[i][f] + (face[f] * (1.0 / weights[i]) - vi)
                    diff[j][f] = diff[j][f] - (face[f] * (1.0 / weights[j]) + vj)
                else:
                    diff[i][f] = diff[i][f] - vi
                    diff[j][f] = diff[j][f] - vj
    return vol, diff


def make_kernel(ngx, ngy, nx, ny, nz):
    weights, deriv, inverse = tables()
    exl, eyl, rows = nx // 4, ny // 4, nx * ny
    total = ngx * ngy
    roots = [(0, 0), (1, 0), (ngx - 1, 0)]
    group = 8 if (nx * eyl) % 8 == 0 else 4

    def kernel(u_in, inc, smooth_out, top_out, st, vol, dif, tq, ysend, yrecv, xrecv, yown, rb, rbr, near,
               bsc, mx, mx2, mxr, myr, xs, xr, ys, yr, bs, br, ms, mr, ns, nr, us, late):
        ix, iy = lax.axis_index("gx"), lax.axis_index("gy")
        loads = [pltpu.make_async_copy(u_in.at[f], st.at[f, BASE:BASE + rows], us) for f in range(5)]
        for c in loads:
            c.start()
        barrier = pltpu.get_barrier_semaphore()
        rank = iy * ngx + ix
        is_root = [rank == y * ngx + x for x, y in roots]
        hub = is_root[-1]
        root = jnp.logical_or(jnp.logical_or(is_root[0], is_root[1]), hub)

        def greet(device):
            pl.semaphore_signal(barrier, 1, device_id=device, device_id_type=MESH)

        def visit(act):
            def step(k, carry):
                t = k + jnp.where(k >= rank, 1, 0)
                act({"gx": lax.rem(t, ngx), "gy": lax.div(t, ngx)})
                return carry

            lax.fori_loop(0, total - 1, step, 0)

        xup, xdn = {"gx": lax.rem(ix + 1, ngx)}, {"gx": lax.rem(ix + ngx - 1, ngx)}
        yup, ydn = {"gy": lax.rem(iy + 1, ngy)}, {"gy": lax.rem(iy + ngy - 1, ngy)}
        inner, wraps = iy > 0, iy == ngy - 1
        for device in (xup, xdn, ydn):
            greet(device)
        pl.when(jnp.logical_not(wraps))(lambda: greet(yup))

        @pl.when(root)
        def _():
            visit(greet)


        def remote(src, dst, ss, rs, dev):
            return pltpu.make_async_remote_copy(
                src_ref=src, dst_ref=dst, send_sem=ss, recv_sem=rs, device_id=dev,
                device_id_type=MESH)

        all_x = remote(xrecv, xrecv, xs, xr, xup)
        all_y = remote(yrecv, yrecv, ys, yr, yup)
        all_blends = remote(rbr, rbr, bs, br, xup)
        others = mxr.at[0:total - 1]
        all_tops = remote(others, others, ms, mr, xup)

        pltpu.make_async_copy(u_in, st.at[0:5, BASE:BASE + rows], us).wait()
        top = None
        for r in range(0, rows, 8):
            here = slice(BASE + r, BASE + r + 8)
            p = mechanics([st[f, here, :] for f in range(5)])
            for f in range(5):
                st[VEL + f, here, :] = p[f]
            speed = jnp.abs(p[0]) + jnp.abs(p[1]) + jnp.abs(p[2]) + 3.0 * p[4]
            top = speed if top is None else jnp.maximum(top, speed)
        mx[...] = jnp.max(top, axis=0, keepdims=True)
        for f in range(5):
            ysend[0, f] = st[f, pl.ds(BASE + ny - 1, nx, ny), :]
            ysend[1, f] = st[f, pl.ds(BASE, nx, ny), :]
        mxr[rank] = mx[...]

        pl.semaphore_wait(barrier, jnp.where(root, 5, 6) + jnp.where(inner, 1, 0))

        @pl.when(wraps)
        def _():
            pl.semaphore_signal(late, 1, device_id=yup, device_id_type=MESH)

        for (x, y), here in zip(roots, is_root):
            @pl.when(jnp.logical_not(here))
            def _():
                remote(mx, mxr.at[rank], ms, mr, {"gx": x, "gy": y}).start()

        remote(ysend.at[0], yrecv.at[0], ys, yr, yup).start()
        pl.when(inner)(lambda: remote(ysend.at[1], yrecv.at[1], ys, yr, ydn).start())
        remote(st.at[0:5, BASE + rows - ny:BASE + rows], xrecv.at[0], xs, xr, xup).start()
        remote(st.at[0:5, BASE:BASE + ny], xrecv.at[1], xs, xr, xdn).start()

        lane = lax.broadcasted_iota(jnp.int32, (8, nz), 1)
        k = lane % 4
        k0, k1, k2, k3 = k == 0, k == 1, k == 2, k == 3

        def lanes(values):
            a, b, c, d = (float(v) for v in values)
            return jnp.where(k0, a, jnp.where(k1, b, jnp.where(k2, c, d))).astype(jnp.float32)

        def roll(x, s):
            return pltpu.roll(x, s % nz, 1)

        zcoef = {s: lanes([inverse[c, c + s] if 0 <= c + s < 4 else 0.0 for c in range(4)])
                 for s in range(-3, 4)}
        for r in range(0, rows, 8):
            here = slice(BASE + r, BASE + r + 8)
            q = st[0, here, :] * st[PRS, here, :]
            t = zcoef[0] * q
            for s in (-3, -2, -1, 1, 2, 3):
                t = t + zcoef[s] * roll(q, -s)
            tq[r:r + 8, :] = t

        ke = k[:eyl]
        for e in range(exl):
            nodes = [[tq[pl.ds((4 * e + i) * ny + j, eyl, 4), :] for j in range(4)]
                     for i in range(4)]
            half = [[sum(float(inverse[a, i]) * nodes[i][j] for i in range(4))
                     for j in range(4)] for a in range(4)]
            e2 = e3 = e4 = 0.0
            for a in range(4):
                for b in range(4):
                    m = sum(float(inverse[b, j]) * half[a][j] for j in range(4))
                    m = m * m
                    e4 = e4 + m
                    if a < 3 and b < 3:
                        e3 = e3 + m
                    if a < 2 and b < 2:
                        e2 = e2 + m
            e3 = jnp.where(ke < 3, e3, 0.0)
            e2 = jnp.where(ke < 2, e2, 0.0)

            def spread(x):
                total = x
                for s in range(1, 4):
                    total = total + jnp.where(ke + s < 4, roll(x, -s), roll(x, 4 - s))
                return total

            e2, e3, e4 = spread(e2), spread(e3), spread(e4)
            energy = jnp.maximum((e4 - e3) / (e4 + 1e-06), (e3 - e2) / (e3 + 1e-06))
            threshold = 0.5 * 10.0 ** (-1.8 * 4.0**0.25)
            sharp = math.log(9999.0) / threshold
            raw = 1.0 / (1.0 + jnp.exp(-sharp * (energy - threshold)))
            raw = jnp.minimum(raw, 0.5)
            rb[e] = raw
        remote(rb, rbr.at[2], bs, br, yup).start()
        pl.when(inner)(lambda: remote(rb, rbr.at[3], bs, br, ydn).start())
        remote(rb, rbr.at[0], bs, br, xup).start()
        remote(rb, rbr.at[1], bs, br, xdn).start()

        for r in range(0, rows, 8):
            here = slice(BASE + r, BASE + r + 8)
            p = logarithms(st[0, here, :], st[PRS, here, :])
            for f in range(3):
                st[LND + f, here, :] = p[f]
        for e in range(exl):
            raw = rb[e]
            close = jnp.maximum(roll(raw, 4), roll(raw, -4))
            if e > 0:
                close = jnp.maximum(close, rb[e - 1])
            if e < exl - 1:
                close = jnp.maximum(close, rb[e + 1])
            near[e, 8:8 + eyl, :] = raw
            near[e, 7:8, :] = raw[0:1]
            near[e, 8 + eyl:9 + eyl, :] = raw[eyl - 1:eyl]
            close = jnp.maximum(close, jnp.maximum(near[e, 7:7 + eyl, :], near[e, 9:9 + eyl, :]))
            bsc[e] = close

        ca = lanes([2 * deriv[0, 1], 2 * deriv[1, 2], 2 * deriv[2, 3], 1 / weights[3]])
        cb = lanes([2 * deriv[1, 0], 2 * deriv[2, 1], 2 * deriv[3, 2], -1 / weights[0]])
        da = lanes([1 / weights[0], 1 / weights[1], 1 / weights[2], 0.0])
        db = lanes([-1 / weights[1], -1 / weights[2], -1 / weights[3], 0.0])
        cam = jnp.where(k3, 0.0, ca)
        cbm = jnp.where(k3, 0.0, cb)
        mc = lanes([2 * deriv[0, 2], 2 * deriv[1, 3], 0.0, 2 * deriv[3, 0]])
        mr_ = lanes([2 * deriv[0, 3], 0.0, 2 * deriv[2, 0], 2 * deriv[3, 1]])

        def z_group(g, carry):
            row = g * 8
            own = [st[f, pl.ds(row + BASE, 8), :] for f in range(FIELDS)]
            nxt = [roll(x, -1) for x in own]
            far = [None] * FIELDS
            for f in (0, 5, 6, 7, PRS, LND, LNR, RAT):
                far[f] = jnp.where(k < 2, roll(own[f], -2), roll(own[f], 3))
            f1 = entropy_flux(own, nxt, 2)
            g1 = dissipated(f1, own, nxt, 2)
            fm = entropy_flux(own, far, 2)
            for f in range(5):
                sel = jnp.where(k3, g1[f], f1[f])
                mm = mc * fm[f] + mr_ * jnp.where(k0, roll(fm[f], -3), roll(fm[f], 2))
                vol[f, pl.ds(row, 8), :] = ca * sel + roll(cb * sel, 1) + mm
                dif[f, pl.ds(row, 8), :] = (
                    (da * g1[f] - cam * f1[f]) + roll(db * g1[f] - cbm * f1[f], 1) - mm)
            return carry

        for g in range(rows // 8):
            z_group(g, 0)

        for e in range(exl):
            for h in range(0, ny, 8):
                slabs = [(4 * e + i) * ny + h for i in range(4)]
                nodes = [[st[f, BASE + r:BASE + r + 8, :] for f in range(FIELDS)] for r in slabs]
                va, da_ = line_terms(nodes, 0, weights, deriv)
                for i in range(4):
                    for f in range(5):
                        vol[f, slabs[i]:slabs[i] + 8, :] += va[i][f]
                        dif[f, slabs[i]:slabs[i] + 8, :] += da_[i][f]
        for g in range(0, nx * eyl, group):
            def rows_of(ref, f, i, base):
                return ref[f, pl.ds(base + 4 * g + i, group, 4), :]

            nodes = [[rows_of(st, f, i, BASE) for f in range(FIELDS)] for i in range(4)]
            va, da_ = line_terms(nodes, 1, weights, deriv)
            for i in range(4):
                for f in range(5):
                    vol[f, pl.ds(4 * g + i, group, 4), :] += va[i][f]
                    dif[f, pl.ds(4 * g + i, group, 4), :] += da_[i][f]

        for e in range(1, exl):
            for h in range(0, ny, 8):
                r = 4 * e * ny + h
                a = [st[f, BASE + r - ny:BASE + r - ny + 8, :] for f in range(FIELDS)]
                b = [st[f, BASE + r:BASE + r + 8, :] for f in range(FIELDS)]
                face = dissipated(entropy_flux(a, b, 0), a, b, 0)
                for f in range(5):
                    vol[f, r - ny:r - ny + 8, :] += face[f] * (1.0 / weights[3])
                    vol[f, r:r + 8, :] -= face[f] * (1.0 / weights[0])
        for g in range(0, nx * eyl, group):
            ye = (lax.broadcasted_iota(jnp.int32, (group, nz), 0) + g) % eyl
            inside = ye < eyl - 1
            a = [st[f, pl.ds(BASE + 4 * g + 3, group, 4), :] for f in range(FIELDS)]
            b = [st[f, pl.ds(BASE + 4 * g + 4, group, 4), :] for f in range(FIELDS)]
            face = dissipated(entropy_flux(a, b, 1), a, b, 1)
            for f in range(5):
                kept = jnp.where(inside, face[f], 0.0)
                vol[f, pl.ds(4 * g + 3, group, 4), :] += kept * (1.0 / weights[3])
                vol[f, pl.ds(4 * g + 4, group, 4), :] -= kept * (1.0 / weights[0])
        for f in range(FIELDS):
            yown[f, 0:nx] = st[f, pl.ds(BASE, nx, ny), :]
            yown[f, nx:2 * nx] = st[f, pl.ds(BASE + ny - 1, nx, ny), :]

        @pl.when(jnp.logical_not(inner))
        def _():
            pl.semaphore_wait(late, 1)
            remote(ysend.at[1], yrecv.at[1], ys, yr, ydn).start()
            remote(rb, rbr.at[3], bs, br, ydn).start()

        all_x.wait_recv()
        for h in range(0, ny, 8):
            for side in range(2):
                got = primitives([xrecv[side, f, h:h + 8, :] for f in range(5)])
                r = h if side == 0 else rows - ny + h
                own = [st[f, BASE + r:BASE + r + 8, :] for f in range(FIELDS)]
                a, b = (got, own) if side == 0 else (own, got)
                face = dissipated(entropy_flux(a, b, 0), a, b, 0)
                scale = -1.0 / weights[0] if side == 0 else 1.0 / weights[3]
                for f in range(5):
                    vol[f, r:r + 8, :] += face[f] * scale

        all_y.wait_recv()
        all_blends.wait_recv()
        row = lax.broadcasted_iota(jnp.int32, (eyl, nz), 0)
        pick = (lax.broadcasted_iota(jnp.int32, (nz, nz // 4), 0)
                == 4 * lax.broadcasted_iota(jnp.int32, (nz, nz // 4), 1)).astype(jnp.float32)
        for e in range(exl):
            close = bsc[e]
            if e == 0:
                close = jnp.maximum(close, rbr[0, exl - 1])
            if e == exl - 1:
                close = jnp.maximum(close, rbr[1, 0])
            close = jnp.maximum(close, jnp.where(row == 0, rbr[2, e, eyl - 1:eyl, :], 0.0))
            close = jnp.maximum(close, jnp.where(row == eyl - 1, rbr[3, e, 0:1, :], 0.0))
            smooth = jnp.maximum(rb[e], 0.5 * close)
            bsc[e] = smooth
            smooth_out[e] = jnp.dot(smooth, pick, precision=lax.Precision.HIGHEST,
                                    preferred_element_type=jnp.float32)

        got = primitives([jnp.concatenate([yrecv[0, f], yrecv[1, f]], axis=0) for f in range(5)])
        own = [yown[f] for f in range(FIELDS)]
        first = lax.broadcasted_iota(jnp.int32, (2 * nx, nz), 0) < nx
        a = [jnp.where(first, got[f], own[f]) for f in range(FIELDS)]
        b = [jnp.where(first, own[f], got[f]) for f in range(FIELDS)]
        face = dissipated(entropy_flux(a, b, 1), a, b, 1)
        for f in range(5):
            vol[f, pl.ds(0, nx, ny), :] -= face[f][:nx] * (1.0 / weights[0])
            vol[f, pl.ds(ny - 1, nx, ny), :] += face[f][nx:] * (1.0 / weights[3])
        under = lax.broadcasted_iota(jnp.int32, (8, nz), 0) < 4
        for e in range(exl):
            for h in range(0, ny, 8):
                y = h // 4
                b = jnp.where(under, bsc[e, y:y + 1, :], bsc[e, y + 1:y + 2, :])
                for i in range(4):
                    r = (4 * e + i) * ny + h
                    for f in range(5):
                        inc[f, r:r + 8, :] = vol[f, r:r + 8, :] + b * dif[f, r:r + 8, :]
        for c in (all_x, all_y, all_blends):
            c.wait_send()

        for here in is_root:
            @pl.when(jnp.logical_not(here))
            def _():
                remote(mx, mxr.at[rank], ms, mr, xup).wait_send()

        @pl.when(root)
        def _():
            all_tops.wait_recv()
            tops = [mxr[i] for i in range(total)]
            while len(tops) > 1:
                pairs = [jnp.maximum(a, b) for a, b in zip(tops[::2], tops[1::2])]
                tops = pairs + tops[2 * len(pairs):]
            top_out[...] = tops[0]

            @pl.when(hub)
            def _():
                mx2[...] = tops[0]

                def spread(x, y):
                    return remote(mx2, myr, ns, nr, {"gx": x, "gy": y})

                for y in range(min(ngy, 64 // ngx)):
                    for x in range(ngx):
                        if (x, y) not in roots:
                            spread(x, y).start()

                def send(t, carry):
                    spread(lax.rem(t, ngx), lax.div(t, ngx)).start()
                    return carry

                def sent(t, carry):
                    spread(0, 0).wait_send()
                    return carry

                if total > 64:
                    lax.fori_loop(64 // ngx * ngx, total, send, 0)
                lax.fori_loop(0, total - len(roots), sent, 0)

        @pl.when(jnp.logical_not(root))
        def _():
            remote(mx2, myr, ns, nr, xup).wait_recv()
            top_out[...] = myr[...]

    f32 = jnp.float32
    dma = pltpu.SemaphoreType.DMA
    pad = BASE + rows + 8
    scratch = [
        pltpu.VMEM((FIELDS, pad, nz), f32),
        pltpu.VMEM((5, rows + 8, nz), f32),
        pltpu.VMEM((5, rows, nz), f32),
        pltpu.VMEM((rows, nz), f32),
        pltpu.VMEM((2, 5, nx, nz), f32),
        pltpu.VMEM((2, 5, nx, nz), f32),
        pltpu.VMEM((2, 5, ny, nz), f32),
        pltpu.VMEM((FIELDS, 2 * nx, nz), f32),
        pltpu.VMEM((exl, eyl, nz), f32),
        pltpu.VMEM((4, exl, eyl, nz), f32),
        pltpu.VMEM((exl, eyl + 16, nz), f32),
        pltpu.VMEM((exl, eyl, nz), f32),
        pltpu.VMEM((1, nz), f32),
        pltpu.VMEM((1, nz), f32),
        pltpu.VMEM((total, 1, nz), f32),
        pltpu.VMEM((1, nz), f32),
        dma, dma, dma, dma, dma, dma,
        dma, dma, dma, dma, dma,
        pltpu.SemaphoreType.REGULAR,
    ]
    return kernel, scratch


def finish(raw, smooth, top, inc, bl):
    step = -0.25 / jnp.max(top[...], axis=(0, 1), keepdims=True)
    for f in range(5):
        inc[f] = step * raw[f]
    bl[...] = smooth[...]


def solution(mesh):
    ngx, ngy = mesh.shape["gx"], mesh.shape["gy"]

    def body(conserved):
        _, nx, ny, nz = conserved.shape
        kernel, scratch = make_kernel(ngx, ngy, nx, ny, nz)
        vmem = pl.BlockSpec(memory_space=pltpu.VMEM)
        shape = lambda *dims: jax.ShapeDtypeStruct(dims, jnp.float32)
        raw, smooth, top = pl.pallas_call(
            kernel,
            out_shape=(shape(5, nx * ny, nz), shape(nx // 4, ny // 4, nz // 4), shape(1, nz)),
            in_specs=[pl.BlockSpec(memory_space=pltpu.HBM)],
            out_specs=(vmem, vmem, vmem),
            scratch_shapes=scratch,
            compiler_params=pltpu.CompilerParams(
                collective_id=0, has_side_effects=True, vmem_limit_bytes=12 * 2**20),
            name="section",
        )(pltpu.with_memory_space_constraint(
            conserved.reshape(5, nx * ny, nz), pltpu.HBM))
        inc, blending = pl.pallas_call(
            finish,
            out_shape=(shape(5, nx * ny, nz), shape(nx // 4, ny // 4, nz // 4)),
            in_specs=[vmem, vmem, vmem],
            out_specs=(vmem, vmem),
            compiler_params=pltpu.CompilerParams(vmem_limit_bytes=8 * 2**20),
            name="finish",
        )(raw, smooth, top)
        return inc.reshape(conserved.shape), blending

    return jax.shard_map(
        body, mesh=mesh, in_specs=(P(None, "gx", "gy", None),),
        out_specs=(P(None, "gx", "gy", None), P("gx", "gy", None)), check_vma=False)
```

```python
import math

import jax
import jax.numpy as jnp
import numpy as np
from jax import lax
from jax.experimental import pallas as pl
from jax.experimental.pallas import tpu as pltpu
from jax.sharding import PartitionSpec as P

gas_gamma = 1.4
MESH = pl.DeviceIdType.MESH
BASE = 8
VEL, PRS, SND, LND, LNR, RAT = 5, 8, 9, 10, 11, 12
FIELDS = 13


def tables():
    inverse_root = 1.0 / math.sqrt(5.0)
    points = np.array([-1.0, -inverse_root, inverse_root, 1.0])
    weights = [1.0 / 6.0, 5.0 / 6.0, 5.0 / 6.0, 1.0 / 6.0]
    barycentric = np.array(
        [
            1.0 / np.prod([points[target] - points[other] for other in range(4) if other != target])
            for target in range(4)
        ]
    )
    derivative = np.zeros((4, 4))
    for target in range(4):
        for source in range(4):
            if target != source:
                derivative[target, source] = (
                    barycentric[source] / barycentric[target] / (points[target] - points[source])
                )
    legendre = np.stack(
        [np.ones(4), points, (3.0 * points**2 - 1.0) / 2.0, (5.0 * points**3 - 3.0 * points) / 2.0],
        1,
    )
    legendre = legendre * np.sqrt(np.arange(4) + 0.5)
    weight_column = np.array(weights)[:, None]
    discrete_norms = np.sum(weight_column * legendre * legendre, 0)
    inverse = (weight_column * legendre).T / discrete_norms[:, None]
    return (weights, derivative, inverse)


def mechanics(conserved):
    density, m1, m2, m3, energy = conserved
    inverse = 1.0 / density
    v1, v2, v3 = m1 * inverse, m2 * inverse, m3 * inverse
    pressure = (gas_gamma - 1.0) * (energy - 0.5 * density * (v1 * v1 + v2 * v2 + v3 * v3))
    sound = jnp.sqrt(gas_gamma * pressure * inverse)
    return [v1, v2, v3, pressure, sound]


def logarithms(density, pressure):
    ratio = density / pressure
    return [jnp.log(density), jnp.log(ratio), ratio]


def primitives(conserved):
    motion = mechanics(conserved)
    return list(conserved) + motion + logarithms(conserved[0], motion[3])


def mean_parts(a, b, log_a, log_b):
    total, gap = a + b, a - b
    relative = gap / total
    square = relative * relative
    small = square < 0.01
    series = 2.0 + square * (2.0 / 3.0 + square * (2.0 / 5.0 + square * (2.0 / 7.0)))
    return jnp.where(small, total, gap), jnp.where(small, series, log_a - log_b)


def entropy_flux(a, b, normal):
    num, den = mean_parts(a[0], b[0], a[LND], b[LND])
    mean_density = num / den
    num, den = mean_parts(a[RAT], b[RAT], a[LNR], b[LNR])
    inverse_beta = den / num
    velocity = [0.5 * (a[VEL + i] + b[VEL + i]) for i in range(3)]
    pressure = 0.5 * (a[PRS] + b[PRS])
    product = 0.5 * (a[5] * b[5] + a[6] * b[6] + a[7] * b[7])
    mass = mean_density * velocity[normal]
    out = [mass]
    for other in range(3):
        momentum = mass * velocity[other]
        out.append(momentum + pressure if other == normal else momentum)
    out.append(
        mass * (product + inverse_beta * (1.0 / (gas_gamma - 1.0)))
        + 0.5 * (a[PRS] * b[VEL + normal] + b[PRS] * a[VEL + normal])
    )
    return out


def dissipated(flux, a, b, normal):
    half = 0.5 * jnp.maximum(
        jnp.abs(a[VEL + normal]) + a[SND], jnp.abs(b[VEL + normal]) + b[SND]
    )
    return [flux[i] - half * (b[i] - a[i]) for i in range(5)]


def line_terms(nodes, normal, weights, deriv):
    vol = [[0.0] * 5 for _ in range(4)]
    diff = [[0.0] * 5 for _ in range(4)]
    for i in range(4):
        for j in range(i + 1, 4):
            flux = entropy_flux(nodes[i], nodes[j], normal)
            ci, cj = 2.0 * float(deriv[i, j]), 2.0 * float(deriv[j, i])
            if j == i + 1:
                face = dissipated(flux, nodes[i], nodes[j], normal)
            for f in range(5):
                vi, vj = ci * flux[f], cj * flux[f]
                vol[i][f] = vol[i][f] + vi
                vol[j][f] = vol[j][f] + vj
                if j == i + 1:
                    diff[i][f] = diff[i][f] + (face[f] * (1.0 / weights[i]) - vi)
                    diff[j][f] = diff[j][f] - (face[f] * (1.0 / weights[j]) + vj)
                else:
                    diff[i][f] = diff[i][f] - vi
                    diff[j][f] = diff[j][f] - vj
    return vol, diff


def make_kernel(ngx, ngy, nx, ny, nz):
    weights, deriv, inverse = tables()
    exl, eyl, rows = nx // 4, ny // 4, nx * ny
    total = ngx * ngy
    parts = 10 * (nx + ny) + 4 * exl * eyl
    roots = [(0, 0), (ngx - 1, 0), (1, 0)]
    group = 8 if (nx * eyl) % 8 == 0 else 4

    def kernel(u_in, inc, smooth_out, top_out, st, vol, dif, tq, ysend, yrecv, xrecv, yown, rb, rbr, near,
               bsc, mx, mx2, mxr, myr, span, sent, halo, tops, late):
        ix, iy = lax.axis_index("gx"), lax.axis_index("gy")
        loads = [pltpu.make_async_copy(u_in.at[f], st.at[f, BASE:BASE + rows], sent) for f in range(5)]
        for c in loads:
            c.start()
        barrier = pltpu.get_barrier_semaphore()
        rank = iy * ngx + ix
        is_root = [rank == y * ngx + x for x, y in roots]
        hub = is_root[1]
        root = jnp.logical_or(jnp.logical_or(is_root[0], is_root[2]), hub)

        def greet(device):
            pl.semaphore_signal(barrier, 1, device_id=device, device_id_type=MESH)

        def visit(act):
            def step(k, carry):
                t = k + jnp.where(k >= rank, 1, 0)
                act({"gx": lax.rem(t, ngx), "gy": lax.div(t, ngx)})
                return carry

            lax.fori_loop(0, total - 1, step, 0)

        xup, xdn = {"gx": lax.rem(ix + 1, ngx)}, {"gx": lax.rem(ix + ngx - 1, ngx)}
        yup, ydn = {"gy": lax.rem(iy + 1, ngy)}, {"gy": lax.rem(iy + ngy - 1, ngy)}
        inner, wraps = iy > 0, iy == ngy - 1
        for device in (xup, xdn, ydn):
            greet(device)
        pl.when(jnp.logical_not(wraps))(lambda: greet(yup))

        @pl.when(root)
        def _():
            visit(greet)


        def remote(src, dst, rs, dev):
            return pltpu.make_async_remote_copy(
                src_ref=src, dst_ref=dst, send_sem=sent, recv_sem=rs, device_id=dev,
                device_id_type=MESH)

        def all_of(ref, count, sem):
            return remote(ref.at[0:count], ref.at[0:count], sem, xup)

        pltpu.make_async_copy(u_in, st.at[0:5, BASE:BASE + rows], sent).wait()
        top = None
        for r in range(0, rows, 8):
            p = mechanics([st[f, BASE + r:BASE + r + 8, :] for f in range(5)])
            speed = jnp.abs(p[0]) + jnp.abs(p[1]) + jnp.abs(p[2]) + 3.0 * p[4]
            top = speed if top is None else jnp.maximum(top, speed)
        mx[...] = jnp.max(top, axis=0, keepdims=True)
        last = jnp.logical_and(wraps, ix >= ngx - 2)

        def meet():
            pl.semaphore_wait(barrier, jnp.where(root, 5, 6) + jnp.where(inner, 1, 0))

            for (x, y), here in zip(roots, is_root):
                @pl.when(jnp.logical_not(here))
                def _():
                    remote(mx, mxr.at[rank], tops, {"gx": x, "gy": y}).start()

        pl.when(last)(meet)
        lane = lax.broadcasted_iota(jnp.int32, (8, nz), 1)
        k = lane % 4
        k0, k1, k2, k3 = k == 0, k == 1, k == 2, k == 3

        def lanes(values):
            a, b, c, d = (float(v) for v in values)
            return jnp.where(k0, a, jnp.where(k1, b, jnp.where(k2, c, d))).astype(jnp.float32)

        def roll(x, s):
            return pltpu.roll(x, s % nz, 1)

        zcoef = {s: lanes([inverse[c, c + s] if 0 <= c + s < 4 else 0.0 for c in range(4)])
                 for s in range(-3, 4)}
        for r in range(0, rows, 8):
            here = slice(BASE + r, BASE + r + 8)
            p = mechanics([st[f, here, :] for f in range(5)])
            for f in range(5):
                st[VEL + f, here, :] = p[f]
            q = st[0, here, :] * p[3]
            t = zcoef[0] * q
            for s in (-3, -2, -1, 1, 2, 3):
                t = t + zcoef[s] * roll(q, -s)
            tq[r:r + 8, :] = t

        ke = k[:eyl]
        for e in range(exl):
            nodes = [[tq[pl.ds((4 * e + i) * ny + j, eyl, 4), :] for j in range(4)]
                     for i in range(4)]
            half = [[sum(float(inverse[a, i]) * nodes[i][j] for i in range(4))
                     for j in range(4)] for a in range(4)]
            e2 = e3 = e4 = 0.0
            for a in range(4):
                for b in range(4):
                    m = sum(float(inverse[b, j]) * half[a][j] for j in range(4))
                    m = m * m
                    e4 = e4 + m
                    if a < 3 and b < 3:
                        e3 = e3 + m
                    if a < 2 and b < 2:
                        e2 = e2 + m
            e3 = jnp.where(ke < 3, e3, 0.0)
            e2 = jnp.where(ke < 2, e2, 0.0)

            def spread(x):
                total = x
                for s in range(1, 4):
                    total = total + jnp.where(ke + s < 4, roll(x, -s), roll(x, 4 - s))
                return total

            e2, e3, e4 = spread(e2), spread(e3), spread(e4)
            energy = jnp.maximum((e4 - e3) / (e4 + 1e-06), (e3 - e2) / (e3 + 1e-06))
            threshold = 0.5 * 10.0 ** (-1.8 * 4.0**0.25)
            sharp = math.log(9999.0) / threshold
            raw = 1.0 / (1.0 + jnp.exp(-sharp * (energy - threshold)))
            raw = jnp.minimum(raw, 0.5)
            rb[e] = raw
        for f in range(5):
            ysend[0, f] = st[f, pl.ds(BASE + ny - 1, nx, ny), :]
            ysend[1, f] = st[f, pl.ds(BASE, nx, ny), :]
        mxr[rank] = mx[...]

        pl.when(jnp.logical_not(last))(meet)
        remote(ysend.at[0], yrecv.at[0], halo, yup).start()
        pl.when(inner)(lambda: remote(ysend.at[1], yrecv.at[1], halo, ydn).start())
        remote(st.at[0:5, BASE + rows - ny:BASE + rows], xrecv.at[0], halo, xup).start()
        remote(st.at[0:5, BASE:BASE + ny], xrecv.at[1], halo, xdn).start()
        remote(rb, rbr.at[2], halo, yup).start()
        pl.when(inner)(lambda: remote(rb, rbr.at[3], halo, ydn).start())
        remote(rb, rbr.at[0], halo, xup).start()
        remote(rb, rbr.at[1], halo, xdn).start()

        @pl.when(wraps)
        def _():
            pl.semaphore_signal(late, 1, device_id=yup, device_id_type=MESH)

        for r in range(0, rows, 8):
            here = slice(BASE + r, BASE + r + 8)
            p = logarithms(st[0, here, :], st[PRS, here, :])
            for f in range(3):
                st[LND + f, here, :] = p[f]
        for e in range(exl):
            raw = rb[e]
            close = jnp.maximum(roll(raw, 4), roll(raw, -4))
            if e > 0:
                close = jnp.maximum(close, rb[e - 1])
            if e < exl - 1:
                close = jnp.maximum(close, rb[e + 1])
            near[e, 8:8 + eyl, :] = raw
            near[e, 7:8, :] = raw[0:1]
            near[e, 8 + eyl:9 + eyl, :] = raw[eyl - 1:eyl]
            close = jnp.maximum(close, jnp.maximum(near[e, 7:7 + eyl, :], near[e, 9:9 + eyl, :]))
            bsc[e] = close

        ca = lanes([2 * deriv[0, 1], 2 * deriv[1, 2], 2 * deriv[2, 3], 1 / weights[3]])
        cb = lanes([2 * deriv[1, 0], 2 * deriv[2, 1], 2 * deriv[3, 2], -1 / weights[0]])
        da = lanes([1 / weights[0], 1 / weights[1], 1 / weights[2], 0.0])
        db = lanes([-1 / weights[1], -1 / weights[2], -1 / weights[3], 0.0])
        cam = jnp.where(k3, 0.0, ca)
        cbm = jnp.where(k3, 0.0, cb)
        mc = lanes([2 * deriv[0, 2], 2 * deriv[1, 3], 0.0, 2 * deriv[3, 0]])
        mr_ = lanes([2 * deriv[0, 3], 0.0, 2 * deriv[2, 0], 2 * deriv[3, 1]])

        def z_group(g, carry):
            row = g * 8
            own = [st[f, pl.ds(row + BASE, 8), :] for f in range(FIELDS)]
            nxt = [roll(x, -1) for x in own]
            far = [None] * FIELDS
            for f in (0, 5, 6, 7, PRS, LND, LNR, RAT):
                far[f] = jnp.where(k < 2, roll(own[f], -2), roll(own[f], 3))
            f1 = entropy_flux(own, nxt, 2)
            g1 = dissipated(f1, own, nxt, 2)
            fm = entropy_flux(own, far, 2)
            for f in range(5):
                sel = jnp.where(k3, g1[f], f1[f])
                mm = mc * fm[f] + mr_ * jnp.where(k0, roll(fm[f], -3), roll(fm[f], 2))
                vol[f, pl.ds(row, 8), :] = ca * sel + roll(cb * sel, 1) + mm
                dif[f, pl.ds(row, 8), :] = (
                    (da * g1[f] - cam * f1[f]) + roll(db * g1[f] - cbm * f1[f], 1) - mm)
            return carry

        for g in range(rows // 8):
            z_group(g, 0)

        for e in range(exl):
            for h in range(0, ny, 8):
                slabs = [(4 * e + i) * ny + h for i in range(4)]
                nodes = [[st[f, BASE + r:BASE + r + 8, :] for f in range(FIELDS)] for r in slabs]
                va, da_ = line_terms(nodes, 0, weights, deriv)
                for i in range(4):
                    for f in range(5):
                        vol[f, slabs[i]:slabs[i] + 8, :] += va[i][f]
                        dif[f, slabs[i]:slabs[i] + 8, :] += da_[i][f]
        for g in range(0, nx * eyl, group):
            def rows_of(ref, f, i, base):
                return ref[f, pl.ds(base + 4 * g + i, group, 4), :]

            nodes = [[rows_of(st, f, i, BASE) for f in range(FIELDS)] for i in range(4)]
            va, da_ = line_terms(nodes, 1, weights, deriv)
            for i in range(4):
                for f in range(5):
                    vol[f, pl.ds(4 * g + i, group, 4), :] += va[i][f]
                    dif[f, pl.ds(4 * g + i, group, 4), :] += da_[i][f]

        for e in range(1, exl):
            for h in range(0, ny, 8):
                r = 4 * e * ny + h
                a = [st[f, BASE + r - ny:BASE + r - ny + 8, :] for f in range(FIELDS)]
                b = [st[f, BASE + r:BASE + r + 8, :] for f in range(FIELDS)]
                face = dissipated(entropy_flux(a, b, 0), a, b, 0)
                for f in range(5):
                    vol[f, r - ny:r - ny + 8, :] += face[f] * (1.0 / weights[3])
                    vol[f, r:r + 8, :] -= face[f] * (1.0 / weights[0])
        for g in range(0, nx * eyl, group):
            ye = (lax.broadcasted_iota(jnp.int32, (group, nz), 0) + g) % eyl
            inside = ye < eyl - 1
            a = [st[f, pl.ds(BASE + 4 * g + 3, group, 4), :] for f in range(FIELDS)]
            b = [st[f, pl.ds(BASE + 4 * g + 4, group, 4), :] for f in range(FIELDS)]
            face = dissipated(entropy_flux(a, b, 1), a, b, 1)
            for f in range(5):
                kept = jnp.where(inside, face[f], 0.0)
                vol[f, pl.ds(4 * g + 3, group, 4), :] += kept * (1.0 / weights[3])
                vol[f, pl.ds(4 * g + 4, group, 4), :] -= kept * (1.0 / weights[0])
        for f in range(FIELDS):
            yown[f, 0:nx] = st[f, pl.ds(BASE, nx, ny), :]
            yown[f, nx:2 * nx] = st[f, pl.ds(BASE + ny - 1, nx, ny), :]

        @pl.when(jnp.logical_not(inner))
        def _():
            pl.semaphore_wait(late, 1)
            remote(ysend.at[1], yrecv.at[1], halo, ydn).start()
            remote(rb, rbr.at[3], halo, ydn).start()

        all_of(span, parts, halo).wait_recv()
        for h in range(0, ny, 8):
            for side in range(2):
                got = primitives([xrecv[side, f, h:h + 8, :] for f in range(5)])
                r = h if side == 0 else rows - ny + h
                own = [st[f, BASE + r:BASE + r + 8, :] for f in range(FIELDS)]
                a, b = (got, own) if side == 0 else (own, got)
                face = dissipated(entropy_flux(a, b, 0), a, b, 0)
                scale = -1.0 / weights[0] if side == 0 else 1.0 / weights[3]
                for f in range(5):
                    vol[f, r:r + 8, :] += face[f] * scale

        row = lax.broadcasted_iota(jnp.int32, (eyl, nz), 0)
        pick = (lax.broadcasted_iota(jnp.int32, (nz, nz // 4), 0)
                == 4 * lax.broadcasted_iota(jnp.int32, (nz, nz // 4), 1)).astype(jnp.float32)
        for e in range(exl):
            close = bsc[e]
            if e == 0:
                close = jnp.maximum(close, rbr[0, exl - 1])
            if e == exl - 1:
                close = jnp.maximum(close, rbr[1, 0])
            close = jnp.maximum(close, jnp.where(row == 0, rbr[2, e, eyl - 1:eyl, :], 0.0))
            close = jnp.maximum(close, jnp.where(row == eyl - 1, rbr[3, e, 0:1, :], 0.0))
            smooth = jnp.maximum(rb[e], 0.5 * close)
            bsc[e] = smooth
            smooth_out[e] = jnp.dot(smooth, pick, precision=lax.Precision.HIGHEST,
                                    preferred_element_type=jnp.float32)

        got = primitives([jnp.concatenate([yrecv[0, f], yrecv[1, f]], axis=0) for f in range(5)])
        own = [yown[f] for f in range(FIELDS)]
        first = lax.broadcasted_iota(jnp.int32, (2 * nx, nz), 0) < nx
        a = [jnp.where(first, got[f], own[f]) for f in range(FIELDS)]
        b = [jnp.where(first, own[f], got[f]) for f in range(FIELDS)]
        face = dissipated(entropy_flux(a, b, 1), a, b, 1)
        for f in range(5):
            vol[f, pl.ds(0, nx, ny), :] -= face[f][:nx] * (1.0 / weights[0])
            vol[f, pl.ds(ny - 1, nx, ny), :] += face[f][nx:] * (1.0 / weights[3])
        under = lax.broadcasted_iota(jnp.int32, (8, nz), 0) < 4
        for e in range(exl):
            for h in range(0, ny, 8):
                y = h // 4
                b = jnp.where(under, bsc[e, y:y + 1, :], bsc[e, y + 1:y + 2, :])
                for i in range(4):
                    r = (4 * e + i) * ny + h
                    for f in range(5):
                        inc[f, r:r + 8, :] = vol[f, r:r + 8, :] + b * dif[f, r:r + 8, :]
        for here, count in ((root, 2), (jnp.logical_not(root), 3)):
            @pl.when(here)
            def _():
                all_of(span, parts + count, tops).wait_send()

        @pl.when(root)
        def _():
            all_of(mxr, total - 1, tops).wait_recv()
            found = [mxr[i] for i in range(total)]
            while len(found) > 1:
                pairs = [jnp.maximum(a, b) for a, b in zip(found[::2], found[1::2])]
                found = pairs + found[2 * len(pairs):]

            @pl.when(hub)
            def _():
                mx2[...] = found[0]

                def spread(x, y):
                    return remote(mx2, myr, tops, {"gx": x, "gy": y})

                for y in range(min(ngy, 64 // ngx)):
                    for x in range(ngx):
                        if (x, y) not in roots:
                            spread(x, y).start()

                def send(t, carry):
                    spread(lax.rem(t, ngx), lax.div(t, ngx)).start()
                    return carry

                if total > 64:
                    lax.fori_loop(64 // ngx * ngx, total, send, 0)
                all_of(mxr, total - len(roots), tops).wait_send()

            top_out[...] = found[0]

        @pl.when(jnp.logical_not(root))
        def _():
            remote(mx2, myr, tops, xup).wait_recv()
            top_out[...] = myr[...]

    f32 = jnp.float32
    dma = pltpu.SemaphoreType.DMA
    pad = BASE + rows + 8
    scratch = [
        pltpu.VMEM((FIELDS, pad, nz), f32),
        pltpu.VMEM((5, rows + 8, nz), f32),
        pltpu.VMEM((5, rows, nz), f32),
        pltpu.VMEM((rows, nz), f32),
        pltpu.VMEM((2, 5, nx, nz), f32),
        pltpu.VMEM((2, 5, nx, nz), f32),
        pltpu.VMEM((2, 5, ny, nz), f32),
        pltpu.VMEM((FIELDS, 2 * nx, nz), f32),
        pltpu.VMEM((exl, eyl, nz), f32),
        pltpu.VMEM((4, exl, eyl, nz), f32),
        pltpu.VMEM((exl, eyl + 16, nz), f32),
        pltpu.VMEM((exl, eyl, nz), f32),
        pltpu.VMEM((1, nz), f32),
        pltpu.VMEM((1, nz), f32),
        pltpu.VMEM((total, 1, nz), f32),
        pltpu.VMEM((1, nz), f32),
        pltpu.VMEM((parts + 3, 1, nz), f32),
        dma, dma, dma,
        pltpu.SemaphoreType.REGULAR,
    ]
    return kernel, scratch


def finish(raw, smooth, top, inc, bl, scaled, done):
    blend = pltpu.make_async_copy(smooth, bl, done)
    blend.start()
    peak = jnp.broadcast_to(top[...], (8, top.shape[1]))
    step = -0.25 / jnp.max(peak, axis=1, keepdims=True)
    for f in range(5):
        for r in range(0, raw.shape[1], 8):
            scaled[f, r:r + 8, :] = step * raw[f, r:r + 8, :]
        pltpu.make_async_copy(scaled.at[f], inc.at[f], done).start()
    pltpu.make_async_copy(scaled, inc, done).wait()
    blend.wait()


def solution(mesh):
    ngx, ngy = mesh.shape["gx"], mesh.shape["gy"]

    def body(conserved):
        _, nx, ny, nz = conserved.shape
        kernel, scratch = make_kernel(ngx, ngy, nx, ny, nz)
        vmem = pl.BlockSpec(memory_space=pltpu.VMEM)
        shape = lambda *dims: jax.ShapeDtypeStruct(dims, jnp.float32)
        raw, smooth, top = pl.pallas_call(
            kernel,
            out_shape=(shape(5, nx * ny, nz), shape(nx // 4, ny // 4, nz // 4), shape(1, nz)),
            in_specs=[pl.BlockSpec(memory_space=pltpu.HBM)],
            out_specs=(vmem, vmem, vmem),
            scratch_shapes=scratch,
            compiler_params=pltpu.CompilerParams(
                collective_id=0, has_side_effects=True, vmem_limit_bytes=12 * 2**20),
            name="section",
        )(pltpu.with_memory_space_constraint(
            conserved.reshape(5, nx * ny, nz), pltpu.HBM))
        inc, blending = pl.pallas_call(
            finish,
            out_shape=(shape(5, nx * ny, nz), shape(nx // 4, ny // 4, nz // 4)),
            in_specs=[vmem, vmem, vmem],
            out_specs=(pl.BlockSpec(memory_space=pltpu.HBM),) * 2,
            scratch_shapes=[pltpu.VMEM((5, nx * ny, nz), jnp.float32), pltpu.SemaphoreType.DMA],
            compiler_params=pltpu.CompilerParams(vmem_limit_bytes=8 * 2**20),
            name="finish",
        )(raw, smooth, top)
        return inc.reshape(conserved.shape), blending

    return jax.shard_map(
        body, mesh=mesh, in_specs=(P(None, "gx", "gy", None),),
        out_specs=(P(None, "gx", "gy", None), P("gx", "gy", None)), check_vma=False)
```

```python
import math

import jax
import jax.numpy as jnp
import numpy as np
from jax import lax
from jax.experimental import pallas as pl
from jax.experimental.pallas import tpu as pltpu
from jax.sharding import PartitionSpec as P

gas_gamma = 1.4
MESH = pl.DeviceIdType.MESH
BASE = 8
VEL, PRS, SND, LND, LNR, RAT = 5, 8, 9, 10, 11, 12
FIELDS = 13


def tables():
    inverse_root = 1.0 / math.sqrt(5.0)
    points = np.array([-1.0, -inverse_root, inverse_root, 1.0])
    weights = [1.0 / 6.0, 5.0 / 6.0, 5.0 / 6.0, 1.0 / 6.0]
    barycentric = np.array(
        [
            1.0 / np.prod([points[target] - points[other] for other in range(4) if other != target])
            for target in range(4)
        ]
    )
    derivative = np.zeros((4, 4))
    for target in range(4):
        for source in range(4):
            if target != source:
                derivative[target, source] = (
                    barycentric[source] / barycentric[target] / (points[target] - points[source])
                )
    legendre = np.stack(
        [np.ones(4), points, (3.0 * points**2 - 1.0) / 2.0, (5.0 * points**3 - 3.0 * points) / 2.0],
        1,
    )
    legendre = legendre * np.sqrt(np.arange(4) + 0.5)
    weight_column = np.array(weights)[:, None]
    discrete_norms = np.sum(weight_column * legendre * legendre, 0)
    inverse = (weight_column * legendre).T / discrete_norms[:, None]
    return (weights, derivative, inverse)


def mechanics(conserved):
    density, m1, m2, m3, energy = conserved
    inverse = 1.0 / density
    v1, v2, v3 = m1 * inverse, m2 * inverse, m3 * inverse
    pressure = (gas_gamma - 1.0) * (energy - 0.5 * density * (v1 * v1 + v2 * v2 + v3 * v3))
    sound = jnp.sqrt(gas_gamma * pressure * inverse)
    return [v1, v2, v3, pressure, sound]


def logarithms(density, pressure):
    ratio = density / pressure
    return [jnp.log(density), jnp.log(ratio), ratio]


def primitives(conserved):
    motion = mechanics(conserved)
    return list(conserved) + motion + logarithms(conserved[0], motion[3])


def mean_parts(a, b, log_a, log_b):
    total, gap = a + b, a - b
    relative = gap / total
    square = relative * relative
    small = square < 0.01
    series = 2.0 + square * (2.0 / 3.0 + square * (2.0 / 5.0 + square * (2.0 / 7.0)))
    return jnp.where(small, total, gap), jnp.where(small, series, log_a - log_b)


def entropy_flux(a, b, normal):
    num, den = mean_parts(a[0], b[0], a[LND], b[LND])
    mean_density = num / den
    num, den = mean_parts(a[RAT], b[RAT], a[LNR], b[LNR])
    inverse_beta = den / num
    velocity = [0.5 * (a[VEL + i] + b[VEL + i]) for i in range(3)]
    pressure = 0.5 * (a[PRS] + b[PRS])
    product = 0.5 * (a[5] * b[5] + a[6] * b[6] + a[7] * b[7])
    mass = mean_density * velocity[normal]
    out = [mass]
    for other in range(3):
        momentum = mass * velocity[other]
        out.append(momentum + pressure if other == normal else momentum)
    out.append(
        mass * (product + inverse_beta * (1.0 / (gas_gamma - 1.0)))
        + 0.5 * (a[PRS] * b[VEL + normal] + b[PRS] * a[VEL + normal])
    )
    return out


def dissipated(flux, a, b, normal):
    half = 0.5 * jnp.maximum(
        jnp.abs(a[VEL + normal]) + a[SND], jnp.abs(b[VEL + normal]) + b[SND]
    )
    return [flux[i] - half * (b[i] - a[i]) for i in range(5)]


def line_terms(nodes, normal, weights, deriv):
    vol = [[0.0] * 5 for _ in range(4)]
    diff = [[0.0] * 5 for _ in range(4)]
    for i in range(4):
        for j in range(i + 1, 4):
            flux = entropy_flux(nodes[i], nodes[j], normal)
            ci, cj = 2.0 * float(deriv[i, j]), 2.0 * float(deriv[j, i])
            if j == i + 1:
                face = dissipated(flux, nodes[i], nodes[j], normal)
            for f in range(5):
                vi, vj = ci * flux[f], cj * flux[f]
                vol[i][f] = vol[i][f] + vi
                vol[j][f] = vol[j][f] + vj
                if j == i + 1:
                    diff[i][f] = diff[i][f] + (face[f] * (1.0 / weights[i]) - vi)
                    diff[j][f] = diff[j][f] - (face[f] * (1.0 / weights[j]) + vj)
                else:
                    diff[i][f] = diff[i][f] - vi
                    diff[j][f] = diff[j][f] - vj
    return vol, diff


def make_kernel(ngx, ngy, nx, ny, nz):
    weights, deriv, inverse = tables()
    exl, eyl, rows = nx // 4, ny // 4, nx * ny
    total = ngx * ngy
    parts = 10 * (nx + ny) + 4 * exl * eyl
    roots = [(0, 0), (ngx - 1, 0), (1, 1), (1, 0)]
    group = 8 if (nx * eyl) % 8 == 0 else 4

    def kernel(u_in, inc, smooth_out, top_out, st, vol, dif, tq, ysend, yrecv, xrecv, yown, rb, rbr, near,
               bsc, mx, mx2, mxr, myr, span, sent, halo, tops, late):
        ix, iy = lax.axis_index("gx"), lax.axis_index("gy")
        loads = [pltpu.make_async_copy(u_in.at[f], st.at[f, BASE:BASE + rows], sent) for f in range(5)]
        for c in loads:
            c.start()
        barrier = pltpu.get_barrier_semaphore()
        rank = iy * ngx + ix
        is_root = [rank == y * ngx + x for x, y in roots]
        root = is_root[0]
        for here in is_root[1:]:
            root = jnp.logical_or(root, here)

        def greet(device):
            pl.semaphore_signal(barrier, 1, device_id=device, device_id_type=MESH)

        def visit(act):
            def step(k, carry):
                t = k + jnp.where(k >= rank, 1, 0)
                act({"gx": lax.rem(t, ngx), "gy": lax.div(t, ngx)})
                return carry

            lax.fori_loop(0, total - 1, step, 0)

        xup, xdn = {"gx": lax.rem(ix + 1, ngx)}, {"gx": lax.rem(ix + ngx - 1, ngx)}
        yup, ydn = {"gy": lax.rem(iy + 1, ngy)}, {"gy": lax.rem(iy + ngy - 1, ngy)}
        inner, wraps = iy > 0, iy == ngy - 1
        need = jnp.where(root, 6, 7) + jnp.where(inner, 1, 0)
        for device in (xup, xdn, ydn):
            greet(device)
        pl.when(jnp.logical_not(wraps))(lambda: greet(yup))

        @pl.when(root)
        def _():
            visit(greet)


        def remote(src, dst, rs, dev):
            return pltpu.make_async_remote_copy(
                src_ref=src, dst_ref=dst, send_sem=sent, recv_sem=rs, device_id=dev,
                device_id_type=MESH)

        def all_of(ref, count, sem):
            return remote(ref.at[0:count], ref.at[0:count], sem, xup)

        pltpu.make_async_copy(u_in, st.at[0:5, BASE:BASE + rows], sent).wait()
        top = None
        for r in range(0, rows, 8):
            density, m1, m2, m3, energy = [st[f, BASE + r:BASE + r + 8, :] for f in range(5)]
            unit = 1.0 / density
            v1, v2, v3 = m1 * unit, m2 * unit, m3 * unit
            inside = energy - 0.5 * density * (v1 * v1 + v2 * v2 + v3 * v3)
            sound = jnp.sqrt(gas_gamma * (gas_gamma - 1.0) * inside * unit)
            speed = jnp.abs(v1) + jnp.abs(v2) + jnp.abs(v3) + 3.0 * sound
            top = speed if top is None else jnp.maximum(top, speed)
        mx[...] = jnp.max(top, axis=0, keepdims=True)
        last = jnp.logical_and(wraps, ix >= ngx - 2)

        def meet():
            pl.semaphore_wait(barrier, need)

            for (x, y), here in zip(roots, is_root):
                @pl.when(jnp.logical_not(here))
                def _():
                    remote(mx, mxr.at[rank], tops, {"gx": x, "gy": y}).start()

        pl.when(last)(meet)
        lane = lax.broadcasted_iota(jnp.int32, (8, nz), 1)
        k = lane % 4
        k0, k1, k2, k3 = k == 0, k == 1, k == 2, k == 3

        def lanes(values):
            a, b, c, d = (float(v) for v in values)
            return jnp.where(k0, a, jnp.where(k1, b, jnp.where(k2, c, d))).astype(jnp.float32)

        def roll(x, s):
            return pltpu.roll(x, s % nz, 1)

        zcoef = {s: lanes([inverse[c, c + s] if 0 <= c + s < 4 else 0.0 for c in range(4)])
                 for s in range(-3, 4)}
        for r in range(0, rows, 8):
            here = slice(BASE + r, BASE + r + 8)
            p = mechanics([st[f, here, :] for f in range(5)])
            for f in range(5):
                st[VEL + f, here, :] = p[f]
            q = st[0, here, :] * p[3]
            t = zcoef[0] * q
            for s in (-3, -2, -1, 1, 2, 3):
                t = t + zcoef[s] * roll(q, -s)
            tq[r:r + 8, :] = t

        ke = k[:eyl]
        for e in range(exl):
            nodes = [[tq[pl.ds((4 * e + i) * ny + j, eyl, 4), :] for j in range(4)]
                     for i in range(4)]
            half = [[sum(float(inverse[a, i]) * nodes[i][j] for i in range(4))
                     for j in range(4)] for a in range(4)]
            e2 = e3 = e4 = 0.0
            for a in range(4):
                for b in range(4):
                    m = sum(float(inverse[b, j]) * half[a][j] for j in range(4))
                    m = m * m
                    e4 = e4 + m
                    if a < 3 and b < 3:
                        e3 = e3 + m
                    if a < 2 and b < 2:
                        e2 = e2 + m
            e3 = jnp.where(ke < 3, e3, 0.0)
            e2 = jnp.where(ke < 2, e2, 0.0)

            def spread(x):
                total = x
                for s in range(1, 4):
                    total = total + jnp.where(ke + s < 4, roll(x, -s), roll(x, 4 - s))
                return total

            e2, e3, e4 = spread(e2), spread(e3), spread(e4)
            energy = jnp.maximum((e4 - e3) / (e4 + 1e-06), (e3 - e2) / (e3 + 1e-06))
            threshold = 0.5 * 10.0 ** (-1.8 * 4.0**0.25)
            sharp = math.log(9999.0) / threshold
            raw = 1.0 / (1.0 + jnp.exp(-sharp * (energy - threshold)))
            raw = jnp.minimum(raw, 0.5)
            rb[e] = raw
        for f in range(5):
            ysend[0, f] = st[f, pl.ds(BASE + ny - 1, nx, ny), :]
            ysend[1, f] = st[f, pl.ds(BASE, nx, ny), :]
        mxr[rank] = mx[...]

        pl.when(jnp.logical_not(last))(meet)
        remote(ysend.at[0], yrecv.at[0], halo, yup).start()
        pl.when(inner)(lambda: remote(ysend.at[1], yrecv.at[1], halo, ydn).start())
        remote(st.at[0:5, BASE + rows - ny:BASE + rows], xrecv.at[0], halo, xup).start()
        remote(st.at[0:5, BASE:BASE + ny], xrecv.at[1], halo, xdn).start()
        remote(rb, rbr.at[2], halo, yup).start()
        pl.when(inner)(lambda: remote(rb, rbr.at[3], halo, ydn).start())
        remote(rb, rbr.at[0], halo, xup).start()
        remote(rb, rbr.at[1], halo, xdn).start()

        @pl.when(wraps)
        def _():
            pl.semaphore_signal(late, 1, device_id=yup, device_id_type=MESH)

        for r in range(0, rows, 8):
            here = slice(BASE + r, BASE + r + 8)
            p = logarithms(st[0, here, :], st[PRS, here, :])
            for f in range(3):
                st[LND + f, here, :] = p[f]
        for e in range(exl):
            raw = rb[e]
            close = jnp.maximum(roll(raw, 4), roll(raw, -4))
            if e > 0:
                close = jnp.maximum(close, rb[e - 1])
            if e < exl - 1:
                close = jnp.maximum(close, rb[e + 1])
            near[e, 8:8 + eyl, :] = raw
            near[e, 7:8, :] = raw[0:1]
            near[e, 8 + eyl:9 + eyl, :] = raw[eyl - 1:eyl]
            close = jnp.maximum(close, jnp.maximum(near[e, 7:7 + eyl, :], near[e, 9:9 + eyl, :]))
            bsc[e] = close

        ca = lanes([2 * deriv[0, 1], 2 * deriv[1, 2], 2 * deriv[2, 3], 1 / weights[3]])
        cb = lanes([2 * deriv[1, 0], 2 * deriv[2, 1], 2 * deriv[3, 2], -1 / weights[0]])
        da = lanes([1 / weights[0], 1 / weights[1], 1 / weights[2], 0.0])
        db = lanes([-1 / weights[1], -1 / weights[2], -1 / weights[3], 0.0])
        cam = jnp.where(k3, 0.0, ca)
        cbm = jnp.where(k3, 0.0, cb)
        mc = lanes([2 * deriv[0, 2], 2 * deriv[1, 3], 0.0, 2 * deriv[3, 0]])
        mr_ = lanes([2 * deriv[0, 3], 0.0, 2 * deriv[2, 0], 2 * deriv[3, 1]])

        def z_group(g, carry):
            row = g * 8
            own = [st[f, pl.ds(row + BASE, 8), :] for f in range(FIELDS)]
            nxt = [roll(x, -1) for x in own]
            far = [None] * FIELDS
            for f in (0, 5, 6, 7, PRS, LND, LNR, RAT):
                far[f] = jnp.where(k < 2, roll(own[f], -2), roll(own[f], 3))
            f1 = entropy_flux(own, nxt, 2)
            g1 = dissipated(f1, own, nxt, 2)
            fm = entropy_flux(own, far, 2)
            for f in range(5):
                sel = jnp.where(k3, g1[f], f1[f])
                mm = mc * fm[f] + mr_ * jnp.where(k0, roll(fm[f], -3), roll(fm[f], 2))
                vol[f, pl.ds(row, 8), :] = ca * sel + roll(cb * sel, 1) + mm
                dif[f, pl.ds(row, 8), :] = (
                    (da * g1[f] - cam * f1[f]) + roll(db * g1[f] - cbm * f1[f], 1) - mm)
            return carry

        for g in range(rows // 8):
            z_group(g, 0)

        for e in range(exl):
            for h in range(0, ny, 8):
                slabs = [(4 * e + i) * ny + h for i in range(4)]
                nodes = [[st[f, BASE + r:BASE + r + 8, :] for f in range(FIELDS)] for r in slabs]
                va, da_ = line_terms(nodes, 0, weights, deriv)
                for i in range(4):
                    for f in range(5):
                        vol[f, slabs[i]:slabs[i] + 8, :] += va[i][f]
                        dif[f, slabs[i]:slabs[i] + 8, :] += da_[i][f]
        for g in range(0, nx * eyl, group):
            def rows_of(ref, f, i, base):
                return ref[f, pl.ds(base + 4 * g + i, group, 4), :]

            nodes = [[rows_of(st, f, i, BASE) for f in range(FIELDS)] for i in range(4)]
            va, da_ = line_terms(nodes, 1, weights, deriv)
            for i in range(4):
                for f in range(5):
                    vol[f, pl.ds(4 * g + i, group, 4), :] += va[i][f]
                    dif[f, pl.ds(4 * g + i, group, 4), :] += da_[i][f]

        for e in range(1, exl):
            for h in range(0, ny, 8):
                r = 4 * e * ny + h
                a = [st[f, BASE + r - ny:BASE + r - ny + 8, :] for f in range(FIELDS)]
                b = [st[f, BASE + r:BASE + r + 8, :] for f in range(FIELDS)]
                face = dissipated(entropy_flux(a, b, 0), a, b, 0)
                for f in range(5):
                    vol[f, r - ny:r - ny + 8, :] += face[f] * (1.0 / weights[3])
                    vol[f, r:r + 8, :] -= face[f] * (1.0 / weights[0])
        for g in range(0, nx * eyl, group):
            ye = (lax.broadcasted_iota(jnp.int32, (group, nz), 0) + g) % eyl
            inside = ye < eyl - 1
            a = [st[f, pl.ds(BASE + 4 * g + 3, group, 4), :] for f in range(FIELDS)]
            b = [st[f, pl.ds(BASE + 4 * g + 4, group, 4), :] for f in range(FIELDS)]
            face = dissipated(entropy_flux(a, b, 1), a, b, 1)
            for f in range(5):
                kept = jnp.where(inside, face[f], 0.0)
                vol[f, pl.ds(4 * g + 3, group, 4), :] += kept * (1.0 / weights[3])
                vol[f, pl.ds(4 * g + 4, group, 4), :] -= kept * (1.0 / weights[0])
        for f in range(FIELDS):
            yown[f, 0:nx] = st[f, pl.ds(BASE, nx, ny), :]
            yown[f, nx:2 * nx] = st[f, pl.ds(BASE + ny - 1, nx, ny), :]

        @pl.when(jnp.logical_not(inner))
        def _():
            pl.semaphore_wait(late, 1)
            remote(ysend.at[1], yrecv.at[1], halo, ydn).start()
            remote(rb, rbr.at[3], halo, ydn).start()

        all_of(span, parts, halo).wait_recv()
        for h in range(0, ny, 8):
            for side in range(2):
                got = primitives([xrecv[side, f, h:h + 8, :] for f in range(5)])
                r = h if side == 0 else rows - ny + h
                own = [st[f, BASE + r:BASE + r + 8, :] for f in range(FIELDS)]
                a, b = (got, own) if side == 0 else (own, got)
                face = dissipated(entropy_flux(a, b, 0), a, b, 0)
                scale = -1.0 / weights[0] if side == 0 else 1.0 / weights[3]
                for f in range(5):
                    vol[f, r:r + 8, :] += face[f] * scale

        row = lax.broadcasted_iota(jnp.int32, (eyl, nz), 0)
        pick = (lax.broadcasted_iota(jnp.int32, (nz, nz // 4), 0)
                == 4 * lax.broadcasted_iota(jnp.int32, (nz, nz // 4), 1)).astype(jnp.float32)
        for e in range(exl):
            close = bsc[e]
            if e == 0:
                close = jnp.maximum(close, rbr[0, exl - 1])
            if e == exl - 1:
                close = jnp.maximum(close, rbr[1, 0])
            close = jnp.maximum(close, jnp.where(row == 0, rbr[2, e, eyl - 1:eyl, :], 0.0))
            close = jnp.maximum(close, jnp.where(row == eyl - 1, rbr[3, e, 0:1, :], 0.0))
            smooth = jnp.maximum(rb[e], 0.5 * close)
            bsc[e] = smooth
            smooth_out[e] = jnp.dot(smooth, pick, precision=lax.Precision.HIGHEST,
                                    preferred_element_type=jnp.float32)

        got = primitives([jnp.concatenate([yrecv[0, f], yrecv[1, f]], axis=0) for f in range(5)])
        own = [yown[f] for f in range(FIELDS)]
        first = lax.broadcasted_iota(jnp.int32, (2 * nx, nz), 0) < nx
        a = [jnp.where(first, got[f], own[f]) for f in range(FIELDS)]
        b = [jnp.where(first, own[f], got[f]) for f in range(FIELDS)]
        face = dissipated(entropy_flux(a, b, 1), a, b, 1)
        for f in range(5):
            vol[f, pl.ds(0, nx, ny), :] -= face[f][:nx] * (1.0 / weights[0])
            vol[f, pl.ds(ny - 1, nx, ny), :] += face[f][nx:] * (1.0 / weights[3])
        under = lax.broadcasted_iota(jnp.int32, (8, nz), 0) < 4
        for e in range(exl):
            for h in range(0, ny, 8):
                y = h // 4
                b = jnp.where(under, bsc[e, y:y + 1, :], bsc[e, y + 1:y + 2, :])
                for i in range(4):
                    r = (4 * e + i) * ny + h
                    for f in range(5):
                        inc[f, r:r + 8, :] = vol[f, r:r + 8, :] + b * dif[f, r:r + 8, :]
        for here, count in ((root, 3), (jnp.logical_not(root), 4)):
            @pl.when(here)
            def _():
                all_of(span, parts + count, tops).wait_send()

        @pl.when(root)
        def _():
            all_of(mxr, total - 1, tops).wait_recv()
            found = [mxr[i] for i in range(total)]
            while len(found) > 1:
                pairs = [jnp.maximum(a, b) for a, b in zip(found[::2], found[1::2])]
                found = pairs + found[2 * len(pairs):]

            for hub, mine in ((1, lambda x, odd: x >= 2 or not odd), (2, lambda x, odd: x < 2 and odd)):
                @pl.when(is_root[hub])
                def _():
                    mx2[...] = found[0]

                    def send(h, carry):
                        for odd in range(2):
                            for x in range(ngx):
                                if mine(x, odd) and not (isinstance(h, int) and (x, 2 * h + odd) in roots):
                                    remote(mx2, myr, tops, {"gx": x, "gy": 2 * h + odd}).start()
                        return carry

                    for h in range(min(ngy // 2, 16)):
                        send(h, 0)
                    if ngy > 32:
                        lax.fori_loop(16, ngy // 2, send, 0)
                    count = sum(mine(x, y % 2) and (x, y) not in roots
                                for x in range(ngx) for y in range(ngy))
                    all_of(mxr, count, tops).wait_send()

            top_out[...] = found[0]

        @pl.when(jnp.logical_not(root))
        def _():
            remote(mx2, myr, tops, xup).wait_recv()
            top_out[...] = myr[...]

    f32 = jnp.float32
    dma = pltpu.SemaphoreType.DMA
    pad = BASE + rows + 8
    scratch = [
        pltpu.VMEM((FIELDS, pad, nz), f32),
        pltpu.VMEM((5, rows + 8, nz), f32),
        pltpu.VMEM((5, rows, nz), f32),
        pltpu.VMEM((rows, nz), f32),
        pltpu.VMEM((2, 5, nx, nz), f32),
        pltpu.VMEM((2, 5, nx, nz), f32),
        pltpu.VMEM((2, 5, ny, nz), f32),
        pltpu.VMEM((FIELDS, 2 * nx, nz), f32),
        pltpu.VMEM((exl, eyl, nz), f32),
        pltpu.VMEM((4, exl, eyl, nz), f32),
        pltpu.VMEM((exl, eyl + 16, nz), f32),
        pltpu.VMEM((exl, eyl, nz), f32),
        pltpu.VMEM((1, nz), f32),
        pltpu.VMEM((1, nz), f32),
        pltpu.VMEM((total, 1, nz), f32),
        pltpu.VMEM((1, nz), f32),
        pltpu.VMEM((parts + 4, 1, nz), f32),
        dma, dma, dma,
        pltpu.SemaphoreType.REGULAR,
    ]
    return kernel, scratch


def finish(raw, smooth, top, inc, bl, scaled, done):
    blend = pltpu.make_async_copy(smooth, bl, done)
    blend.start()
    peak = jnp.broadcast_to(top[...], (8, top.shape[1]))
    step = -0.25 / jnp.max(peak, axis=1, keepdims=True)
    for f in range(5):
        for r in range(0, raw.shape[1], 8):
            scaled[f, r:r + 8, :] = step * raw[f, r:r + 8, :]
        pltpu.make_async_copy(scaled.at[f], inc.at[f], done).start()
    pltpu.make_async_copy(scaled, inc, done).wait()
    blend.wait()


def solution(mesh):
    ngx, ngy = mesh.shape["gx"], mesh.shape["gy"]

    def body(conserved):
        _, nx, ny, nz = conserved.shape
        kernel, scratch = make_kernel(ngx, ngy, nx, ny, nz)
        vmem = pl.BlockSpec(memory_space=pltpu.VMEM)
        shape = lambda *dims: jax.ShapeDtypeStruct(dims, jnp.float32)
        raw, smooth, top = pl.pallas_call(
            kernel,
            out_shape=(shape(5, nx * ny, nz), shape(nx // 4, ny // 4, nz // 4), shape(1, nz)),
            in_specs=[pl.BlockSpec(memory_space=pltpu.HBM)],
            out_specs=(vmem, vmem, vmem),
            scratch_shapes=scratch,
            compiler_params=pltpu.CompilerParams(
                collective_id=0, has_side_effects=True, vmem_limit_bytes=12 * 2**20),
            name="section",
        )(pltpu.with_memory_space_constraint(
            conserved.reshape(5, nx * ny, nz), pltpu.HBM))
        inc, blending = pl.pallas_call(
            finish,
            out_shape=(shape(5, nx * ny, nz), shape(nx // 4, ny // 4, nz // 4)),
            in_specs=[vmem, vmem, vmem],
            out_specs=(pl.BlockSpec(memory_space=pltpu.HBM),) * 2,
            scratch_shapes=[pltpu.VMEM((5, nx * ny, nz), jnp.float32), pltpu.SemaphoreType.DMA],
            compiler_params=pltpu.CompilerParams(vmem_limit_bytes=8 * 2**20),
            name="finish",
        )(raw, smooth, top)
        return inc.reshape(conserved.shape), blending

    return jax.shard_map(
        body, mesh=mesh, in_specs=(P(None, "gx", "gy", None),),
        out_specs=(P(None, "gx", "gy", None), P("gx", "gy", None)), check_vma=False)
```

```python
import math

import jax
import jax.numpy as jnp
import numpy as np
from jax import lax
from jax.experimental import pallas as pl
from jax.experimental.pallas import tpu as pltpu
from jax.sharding import PartitionSpec as P

gas_gamma = 1.4
MESH = pl.DeviceIdType.MESH
BASE = 8
VEL, PRS, SND, LND, LNR, RAT = 5, 8, 9, 10, 11, 12
FIELDS = 13


def tables():
    inverse_root = 1.0 / math.sqrt(5.0)
    points = np.array([-1.0, -inverse_root, inverse_root, 1.0])
    weights = [1.0 / 6.0, 5.0 / 6.0, 5.0 / 6.0, 1.0 / 6.0]
    barycentric = np.array(
        [
            1.0 / np.prod([points[target] - points[other] for other in range(4) if other != target])
            for target in range(4)
        ]
    )
    derivative = np.zeros((4, 4))
    for target in range(4):
        for source in range(4):
            if target != source:
                derivative[target, source] = (
                    barycentric[source] / barycentric[target] / (points[target] - points[source])
                )
    legendre = np.stack(
        [np.ones(4), points, (3.0 * points**2 - 1.0) / 2.0, (5.0 * points**3 - 3.0 * points) / 2.0],
        1,
    )
    legendre = legendre * np.sqrt(np.arange(4) + 0.5)
    weight_column = np.array(weights)[:, None]
    discrete_norms = np.sum(weight_column * legendre * legendre, 0)
    inverse = (weight_column * legendre).T / discrete_norms[:, None]
    return (weights, derivative, inverse)


def mechanics(conserved):
    density, m1, m2, m3, energy = conserved
    inverse = 1.0 / density
    v1, v2, v3 = m1 * inverse, m2 * inverse, m3 * inverse
    pressure = (gas_gamma - 1.0) * (energy - 0.5 * density * (v1 * v1 + v2 * v2 + v3 * v3))
    sound = jnp.sqrt(gas_gamma * pressure * inverse)
    return [v1, v2, v3, pressure, sound]


def logarithms(density, pressure):
    ratio = density / pressure
    return [jnp.log(density), jnp.log(ratio), ratio]


def primitives(conserved):
    motion = mechanics(conserved)
    return list(conserved) + motion + logarithms(conserved[0], motion[3])


def mean_parts(a, b, log_a, log_b):
    total, gap = a + b, a - b
    relative = gap / total
    square = relative * relative
    small = square < 0.01
    series = 2.0 + square * (2.0 / 3.0 + square * (2.0 / 5.0 + square * (2.0 / 7.0)))
    return jnp.where(small, total, gap), jnp.where(small, series, log_a - log_b)


def entropy_flux(a, b, normal):
    num, den = mean_parts(a[0], b[0], a[LND], b[LND])
    mean_density = num / den
    num, den = mean_parts(a[RAT], b[RAT], a[LNR], b[LNR])
    inverse_beta = den / num
    velocity = [0.5 * (a[VEL + i] + b[VEL + i]) for i in range(3)]
    pressure = 0.5 * (a[PRS] + b[PRS])
    product = 0.5 * (a[5] * b[5] + a[6] * b[6] + a[7] * b[7])
    mass = mean_density * velocity[normal]
    out = [mass]
    for other in range(3):
        momentum = mass * velocity[other]
        out.append(momentum + pressure if other == normal else momentum)
    out.append(
        mass * (product + inverse_beta * (1.0 / (gas_gamma - 1.0)))
        + 0.5 * (a[PRS] * b[VEL + normal] + b[PRS] * a[VEL + normal])
    )
    return out


def dissipated(flux, a, b, normal):
    half = 0.5 * jnp.maximum(
        jnp.abs(a[VEL + normal]) + a[SND], jnp.abs(b[VEL + normal]) + b[SND]
    )
    return [flux[i] - half * (b[i] - a[i]) for i in range(5)]


def line_terms(nodes, normal, weights, deriv):
    vol = [[0.0] * 5 for _ in range(4)]
    diff = [[0.0] * 5 for _ in range(4)]
    for i in range(4):
        for j in range(i + 1, 4):
            flux = entropy_flux(nodes[i], nodes[j], normal)
            ci, cj = 2.0 * float(deriv[i, j]), 2.0 * float(deriv[j, i])
            if j == i + 1:
                face = dissipated(flux, nodes[i], nodes[j], normal)
            for f in range(5):
                vi, vj = ci * flux[f], cj * flux[f]
                vol[i][f] = vol[i][f] + vi
                vol[j][f] = vol[j][f] + vj
                if j == i + 1:
                    diff[i][f] = diff[i][f] + (face[f] * (1.0 / weights[i]) - vi)
                    diff[j][f] = diff[j][f] - (face[f] * (1.0 / weights[j]) + vj)
                else:
                    diff[i][f] = diff[i][f] - vi
                    diff[j][f] = diff[j][f] - vj
    return vol, diff


def make_kernel(ngx, ngy, nx, ny, nz):
    weights, deriv, inverse = tables()
    exl, eyl, rows = nx // 4, ny // 4, nx * ny
    total = ngx * ngy
    parts = 10 * (nx + ny) + 4 * exl * eyl
    roots = [(0, 0), (ngx - 1, 0), (1, 1), (1, 0)]
    group = 8 if (nx * eyl) % 8 == 0 else 4

    def kernel(u_in, inc, smooth_out, top_out, st, vol, dif, tq, ysend, yrecv, xrecv, yown, rb, rbr, near,
               bsc, mx, mx2, mxr, myr, span, sent, halo, tops, late):
        ix, iy = lax.axis_index("gx"), lax.axis_index("gy")
        loads = [pltpu.make_async_copy(u_in.at[f], st.at[f, BASE:BASE + rows], sent) for f in range(5)]
        for c in loads:
            c.start()
        barrier = pltpu.get_barrier_semaphore()
        rank = iy * ngx + ix
        is_root = [rank == y * ngx + x for x, y in roots]
        root = is_root[0]
        for here in is_root[1:]:
            root = jnp.logical_or(root, here)

        def greet(device):
            pl.semaphore_signal(barrier, 1, device_id=device, device_id_type=MESH)

        def visit(act):
            def step(k, carry):
                t = k + jnp.where(k >= rank, 1, 0)
                act({"gx": lax.rem(t, ngx), "gy": lax.div(t, ngx)})
                return carry

            lax.fori_loop(0, total - 1, step, 0)

        xup, xdn = {"gx": lax.rem(ix + 1, ngx)}, {"gx": lax.rem(ix + ngx - 1, ngx)}
        yup, ydn = {"gy": lax.rem(iy + 1, ngy)}, {"gy": lax.rem(iy + ngy - 1, ngy)}
        inner, wraps = iy > 0, iy == ngy - 1
        need = jnp.where(root, 6, 7) + jnp.where(inner, 1, 0)
        for device in (xup, xdn, ydn):
            greet(device)
        pl.when(jnp.logical_not(wraps))(lambda: greet(yup))

        @pl.when(root)
        def _():
            visit(greet)


        def remote(src, dst, rs, dev):
            return pltpu.make_async_remote_copy(
                src_ref=src, dst_ref=dst, send_sem=sent, recv_sem=rs, device_id=dev,
                device_id_type=MESH)

        def all_of(ref, count, sem):
            return remote(ref.at[0:count], ref.at[0:count], sem, xup)

        pltpu.make_async_copy(u_in, st.at[0:5, BASE:BASE + rows], sent).wait()
        top = None
        for r in range(0, rows, 8):
            density, m1, m2, m3, energy = [st[f, BASE + r:BASE + r + 8, :] for f in range(5)]
            unit = 1.0 / density
            v1, v2, v3 = m1 * unit, m2 * unit, m3 * unit
            inside = energy - 0.5 * density * (v1 * v1 + v2 * v2 + v3 * v3)
            sound = jnp.sqrt(gas_gamma * (gas_gamma - 1.0) * inside * unit)
            speed = jnp.abs(v1) + jnp.abs(v2) + jnp.abs(v3) + 3.0 * sound
            top = speed if top is None else jnp.maximum(top, speed)
        mx[...] = jnp.max(top, axis=0, keepdims=True)
        last = jnp.logical_and(wraps, ix >= ngx - 2)

        def meet():
            pl.semaphore_wait(barrier, need)

            for (x, y), here in zip(roots, is_root):
                @pl.when(jnp.logical_not(here))
                def _():
                    remote(mx, mxr.at[rank], tops, {"gx": x, "gy": y}).start()

        pl.when(last)(meet)
        lane = lax.broadcasted_iota(jnp.int32, (8, nz), 1)
        k = lane % 4
        k0, k1, k2, k3 = k == 0, k == 1, k == 2, k == 3

        def lanes(values):
            a, b, c, d = (float(v) for v in values)
            return jnp.where(k0, a, jnp.where(k1, b, jnp.where(k2, c, d))).astype(jnp.float32)

        def roll(x, s):
            return pltpu.roll(x, s % nz, 1)

        zcoef = {s: lanes([inverse[c, c + s] if 0 <= c + s < 4 else 0.0 for c in range(4)])
                 for s in range(-3, 4)}
        for r in range(0, rows, 8):
            here = slice(BASE + r, BASE + r + 8)
            p = mechanics([st[f, here, :] for f in range(5)])
            for f in range(5):
                st[VEL + f, here, :] = p[f]
            q = st[0, here, :] * p[3]
            t = zcoef[0] * q
            for s in (-3, -2, -1, 1, 2, 3):
                t = t + zcoef[s] * roll(q, -s)
            tq[r:r + 8, :] = t

        ke = k[:eyl]
        for e in range(exl):
            nodes = [[tq[pl.ds((4 * e + i) * ny + j, eyl, 4), :] for j in range(4)]
                     for i in range(4)]
            half = [[sum(float(inverse[a, i]) * nodes[i][j] for i in range(4))
                     for j in range(4)] for a in range(4)]
            e2 = e3 = e4 = 0.0
            for a in range(4):
                for b in range(4):
                    m = sum(float(inverse[b, j]) * half[a][j] for j in range(4))
                    m = m * m
                    e4 = e4 + m
                    if a < 3 and b < 3:
                        e3 = e3 + m
                    if a < 2 and b < 2:
                        e2 = e2 + m
            e3 = jnp.where(ke < 3, e3, 0.0)
            e2 = jnp.where(ke < 2, e2, 0.0)

            def spread(x):
                total = x
                for s in range(1, 4):
                    total = total + jnp.where(ke + s < 4, roll(x, -s), roll(x, 4 - s))
                return total

            e2, e3, e4 = spread(e2), spread(e3), spread(e4)
            energy = jnp.maximum((e4 - e3) / (e4 + 1e-06), (e3 - e2) / (e3 + 1e-06))
            threshold = 0.5 * 10.0 ** (-1.8 * 4.0**0.25)
            sharp = math.log(9999.0) / threshold
            raw = 1.0 / (1.0 + jnp.exp(-sharp * (energy - threshold)))
            raw = jnp.minimum(raw, 0.5)
            rb[e] = raw
        for f in range(5):
            ysend[0, f] = st[f, pl.ds(BASE + ny - 1, nx, ny), :]
            ysend[1, f] = st[f, pl.ds(BASE, nx, ny), :]
        mxr[rank] = mx[...]

        pl.when(jnp.logical_not(last))(meet)
        remote(ysend.at[0], yrecv.at[0], halo, yup).start()
        pl.when(inner)(lambda: remote(ysend.at[1], yrecv.at[1], halo, ydn).start())
        remote(st.at[0:5, BASE + rows - ny:BASE + rows], xrecv.at[0], halo, xup).start()
        remote(st.at[0:5, BASE:BASE + ny], xrecv.at[1], halo, xdn).start()
        remote(rb, rbr.at[2], halo, yup).start()
        pl.when(inner)(lambda: remote(rb, rbr.at[3], halo, ydn).start())
        remote(rb, rbr.at[0], halo, xup).start()
        remote(rb, rbr.at[1], halo, xdn).start()

        @pl.when(wraps)
        def _():
            pl.semaphore_signal(late, 1, device_id=yup, device_id_type=MESH)

        for r in range(0, rows, 8):
            here = slice(BASE + r, BASE + r + 8)
            p = logarithms(st[0, here, :], st[PRS, here, :])
            for f in range(3):
                st[LND + f, here, :] = p[f]
        for e in range(exl):
            raw = rb[e]
            close = jnp.maximum(roll(raw, 4), roll(raw, -4))
            if e > 0:
                close = jnp.maximum(close, rb[e - 1])
            if e < exl - 1:
                close = jnp.maximum(close, rb[e + 1])
            near[e, 8:8 + eyl, :] = raw
            near[e, 7:8, :] = raw[0:1]
            near[e, 8 + eyl:9 + eyl, :] = raw[eyl - 1:eyl]
            close = jnp.maximum(close, jnp.maximum(near[e, 7:7 + eyl, :], near[e, 9:9 + eyl, :]))
            bsc[e] = close

        ca = lanes([2 * deriv[0, 1], 2 * deriv[1, 2], 2 * deriv[2, 3], 1 / weights[3]])
        cb = lanes([2 * deriv[1, 0], 2 * deriv[2, 1], 2 * deriv[3, 2], -1 / weights[0]])
        da = lanes([1 / weights[0], 1 / weights[1], 1 / weights[2], 0.0])
        db = lanes([-1 / weights[1], -1 / weights[2], -1 / weights[3], 0.0])
        cam = jnp.where(k3, 0.0, ca)
        cbm = jnp.where(k3, 0.0, cb)
        mc = lanes([2 * deriv[0, 2], 2 * deriv[1, 3], 0.0, 2 * deriv[3, 0]])
        mr_ = lanes([2 * deriv[0, 3], 0.0, 2 * deriv[2, 0], 2 * deriv[3, 1]])

        def z_group(g, carry):
            row = g * 8
            own = [st[f, pl.ds(row + BASE, 8), :] for f in range(FIELDS)]
            nxt = [roll(x, -1) for x in own]
            far = [None] * FIELDS
            for f in (0, 5, 6, 7, PRS, LND, LNR, RAT):
                far[f] = jnp.where(k < 2, roll(own[f], -2), roll(own[f], 3))
            f1 = entropy_flux(own, nxt, 2)
            g1 = dissipated(f1, own, nxt, 2)
            fm = entropy_flux(own, far, 2)
            for f in range(5):
                sel = jnp.where(k3, g1[f], f1[f])
                mm = mc * fm[f] + mr_ * jnp.where(k0, roll(fm[f], -3), roll(fm[f], 2))
                vol[f, pl.ds(row, 8), :] = ca * sel + roll(cb * sel, 1) + mm
                dif[f, pl.ds(row, 8), :] = (
                    (da * g1[f] - cam * f1[f]) + roll(db * g1[f] - cbm * f1[f], 1) - mm)
            return carry

        for g in range(rows // 8):
            z_group(g, 0)

        for e in range(exl):
            for h in range(0, ny, 8):
                slabs = [(4 * e + i) * ny + h for i in range(4)]
                nodes = [[st[f, BASE + r:BASE + r + 8, :] for f in range(FIELDS)] for r in slabs]
                va, da_ = line_terms(nodes, 0, weights, deriv)
                for i in range(4):
                    for f in range(5):
                        vol[f, slabs[i]:slabs[i] + 8, :] += va[i][f]
                        dif[f, slabs[i]:slabs[i] + 8, :] += da_[i][f]
        for g in range(0, nx * eyl, group):
            def rows_of(ref, f, i, base):
                return ref[f, pl.ds(base + 4 * g + i, group, 4), :]

            nodes = [[rows_of(st, f, i, BASE) for f in range(FIELDS)] for i in range(4)]
            va, da_ = line_terms(nodes, 1, weights, deriv)
            for i in range(4):
                for f in range(5):
                    vol[f, pl.ds(4 * g + i, group, 4), :] += va[i][f]
                    dif[f, pl.ds(4 * g + i, group, 4), :] += da_[i][f]

        for e in range(1, exl):
            for h in range(0, ny, 8):
                r = 4 * e * ny + h
                a = [st[f, BASE + r - ny:BASE + r - ny + 8, :] for f in range(FIELDS)]
                b = [st[f, BASE + r:BASE + r + 8, :] for f in range(FIELDS)]
                face = dissipated(entropy_flux(a, b, 0), a, b, 0)
                for f in range(5):
                    vol[f, r - ny:r - ny + 8, :] += face[f] * (1.0 / weights[3])
                    vol[f, r:r + 8, :] -= face[f] * (1.0 / weights[0])
        for g in range(0, nx * eyl, group):
            ye = (lax.broadcasted_iota(jnp.int32, (group, nz), 0) + g) % eyl
            inside = ye < eyl - 1
            a = [st[f, pl.ds(BASE + 4 * g + 3, group, 4), :] for f in range(FIELDS)]
            b = [st[f, pl.ds(BASE + 4 * g + 4, group, 4), :] for f in range(FIELDS)]
            face = dissipated(entropy_flux(a, b, 1), a, b, 1)
            for f in range(5):
                kept = jnp.where(inside, face[f], 0.0)
                vol[f, pl.ds(4 * g + 3, group, 4), :] += kept * (1.0 / weights[3])
                vol[f, pl.ds(4 * g + 4, group, 4), :] -= kept * (1.0 / weights[0])
        for f in range(FIELDS):
            yown[f, 0:nx] = st[f, pl.ds(BASE, nx, ny), :]
            yown[f, nx:2 * nx] = st[f, pl.ds(BASE + ny - 1, nx, ny), :]

        @pl.when(jnp.logical_not(inner))
        def _():
            pl.semaphore_wait(late, 1)
            remote(ysend.at[1], yrecv.at[1], halo, ydn).start()
            remote(rb, rbr.at[3], halo, ydn).start()

        all_of(span, parts, halo).wait_recv()
        for h in range(0, ny, 8):
            for side in range(2):
                got = primitives([xrecv[side, f, h:h + 8, :] for f in range(5)])
                r = h if side == 0 else rows - ny + h
                own = [st[f, BASE + r:BASE + r + 8, :] for f in range(FIELDS)]
                a, b = (got, own) if side == 0 else (own, got)
                face = dissipated(entropy_flux(a, b, 0), a, b, 0)
                scale = -1.0 / weights[0] if side == 0 else 1.0 / weights[3]
                for f in range(5):
                    vol[f, r:r + 8, :] += face[f] * scale

        row = lax.broadcasted_iota(jnp.int32, (eyl, nz), 0)
        pick = (lax.broadcasted_iota(jnp.int32, (nz, nz // 4), 0)
                == 4 * lax.broadcasted_iota(jnp.int32, (nz, nz // 4), 1)).astype(jnp.float32)
        for e in range(exl):
            close = bsc[e]
            if e == 0:
                close = jnp.maximum(close, rbr[0, exl - 1])
            if e == exl - 1:
                close = jnp.maximum(close, rbr[1, 0])
            close = jnp.maximum(close, jnp.where(row == 0, rbr[2, e, eyl - 1:eyl, :], 0.0))
            close = jnp.maximum(close, jnp.where(row == eyl - 1, rbr[3, e, 0:1, :], 0.0))
            smooth = jnp.maximum(rb[e], 0.5 * close)
            bsc[e] = smooth
            smooth_out[e] = jnp.dot(smooth, pick, precision=lax.Precision.HIGHEST,
                                    preferred_element_type=jnp.float32)

        got = primitives([jnp.concatenate([yrecv[0, f], yrecv[1, f]], axis=0) for f in range(5)])
        own = [yown[f] for f in range(FIELDS)]
        first = lax.broadcasted_iota(jnp.int32, (2 * nx, nz), 0) < nx
        a = [jnp.where(first, got[f], own[f]) for f in range(FIELDS)]
        b = [jnp.where(first, own[f], got[f]) for f in range(FIELDS)]
        face = dissipated(entropy_flux(a, b, 1), a, b, 1)
        for f in range(5):
            vol[f, pl.ds(0, nx, ny), :] -= face[f][:nx] * (1.0 / weights[0])
            vol[f, pl.ds(ny - 1, nx, ny), :] += face[f][nx:] * (1.0 / weights[3])
        under = lax.broadcasted_iota(jnp.int32, (8, nz), 0) < 4
        for e in range(exl):
            for h in range(0, ny, 8):
                y = h // 4
                b = jnp.where(under, bsc[e, y:y + 1, :], bsc[e, y + 1:y + 2, :])
                for i in range(4):
                    r = (4 * e + i) * ny + h
                    for f in range(5):
                        inc[f, r:r + 8, :] = vol[f, r:r + 8, :] + b * dif[f, r:r + 8, :]
        for here, count in ((root, 3), (jnp.logical_not(root), 4)):
            @pl.when(here)
            def _():
                all_of(span, parts + count, tops).wait_send()

        def gather():
            all_of(mxr, total - 1, tops).wait_recv()
            found = [mxr[i] for i in range(total)]
            while len(found) > 1:
                pairs = [jnp.maximum(a, b) for a, b in zip(found[::2], found[1::2])]
                found = pairs + found[2 * len(pairs):]
            return found[0]

        for hub, mine in ((1, lambda x, odd: x >= 2 or not odd), (2, lambda x, odd: x < 2 and odd)):
            @pl.when(is_root[hub])
            def _():
                mx2[...] = gather()

                def send(h, carry):
                    for odd in range(2):
                        for x in range(ngx):
                            if mine(x, odd) and not (isinstance(h, int) and (x, 2 * h + odd) in roots):
                                remote(mx2, myr, tops, {"gx": x, "gy": 2 * h + odd}).start()
                    return carry

                for h in range(min(ngy // 2, 16)):
                    send(h, 0)
                if ngy > 32:
                    lax.fori_loop(16, ngy // 2, send, 0)
                top_out[...] = mx2[...]
                count = sum(mine(x, y % 2) and (x, y) not in roots
                            for x in range(ngx) for y in range(ngy))
                all_of(mxr, count, tops).wait_send()

        @pl.when(jnp.logical_not(root))
        def _():
            remote(mx2, myr, tops, xup).wait_recv()
            top_out[...] = myr[...]

        @pl.when(jnp.logical_or(is_root[0], is_root[3]))
        def _():
            top_out[...] = gather()

    f32 = jnp.float32
    dma = pltpu.SemaphoreType.DMA
    pad = BASE + rows + 8
    scratch = [
        pltpu.VMEM((FIELDS, pad, nz), f32),
        pltpu.VMEM((5, rows + 8, nz), f32),
        pltpu.VMEM((5, rows, nz), f32),
        pltpu.VMEM((rows, nz), f32),
        pltpu.VMEM((2, 5, nx, nz), f32),
        pltpu.VMEM((2, 5, nx, nz), f32),
        pltpu.VMEM((2, 5, ny, nz), f32),
        pltpu.VMEM((FIELDS, 2 * nx, nz), f32),
        pltpu.VMEM((exl, eyl, nz), f32),
        pltpu.VMEM((4, exl, eyl, nz), f32),
        pltpu.VMEM((exl, eyl + 16, nz), f32),
        pltpu.VMEM((exl, eyl, nz), f32),
        pltpu.VMEM((1, nz), f32),
        pltpu.VMEM((1, nz), f32),
        pltpu.VMEM((total, 1, nz), f32),
        pltpu.VMEM((1, nz), f32),
        pltpu.VMEM((parts + 4, 1, nz), f32),
        dma, dma, dma,
        pltpu.SemaphoreType.REGULAR,
    ]
    return kernel, scratch


def finish(raw, smooth, top, inc, bl, scaled, done):
    blend = pltpu.make_async_copy(smooth, bl, done)
    blend.start()
    peak = jnp.broadcast_to(top[...], (8, top.shape[1]))
    step = -0.25 / jnp.max(peak, axis=1, keepdims=True)
    for f in range(5):
        for r in range(0, raw.shape[1], 8):
            scaled[f, r:r + 8, :] = step * raw[f, r:r + 8, :]
        pltpu.make_async_copy(scaled.at[f], inc.at[f], done).start()
    pltpu.make_async_copy(scaled, inc, done).wait()
    blend.wait()


def solution(mesh):
    ngx, ngy = mesh.shape["gx"], mesh.shape["gy"]

    def body(conserved):
        _, nx, ny, nz = conserved.shape
        kernel, scratch = make_kernel(ngx, ngy, nx, ny, nz)
        vmem = pl.BlockSpec(memory_space=pltpu.VMEM)
        shape = lambda *dims: jax.ShapeDtypeStruct(dims, jnp.float32)
        raw, smooth, top = pl.pallas_call(
            kernel,
            out_shape=(shape(5, nx * ny, nz), shape(nx // 4, ny // 4, nz // 4), shape(1, nz)),
            in_specs=[pl.BlockSpec(memory_space=pltpu.HBM)],
            out_specs=(vmem, vmem, vmem),
            scratch_shapes=scratch,
            compiler_params=pltpu.CompilerParams(
                collective_id=0, has_side_effects=True, vmem_limit_bytes=12 * 2**20),
            name="section",
        )(pltpu.with_memory_space_constraint(
            conserved.reshape(5, nx * ny, nz), pltpu.HBM))
        inc, blending = pl.pallas_call(
            finish,
            out_shape=(shape(5, nx * ny, nz), shape(nx // 4, ny // 4, nz // 4)),
            in_specs=[vmem, vmem, vmem],
            out_specs=(pl.BlockSpec(memory_space=pltpu.HBM),) * 2,
            scratch_shapes=[pltpu.VMEM((5, nx * ny, nz), jnp.float32), pltpu.SemaphoreType.DMA],
            compiler_params=pltpu.CompilerParams(vmem_limit_bytes=8 * 2**20),
            name="finish",
        )(raw, smooth, top)
        return inc.reshape(conserved.shape), blending

    return jax.shard_map(
        body, mesh=mesh, in_specs=(P(None, "gx", "gy", None),),
        out_specs=(P(None, "gx", "gy", None), P("gx", "gy", None)), check_vma=False)
```

```python
import math

import jax
import jax.numpy as jnp
import numpy as np
from jax import lax
from jax.experimental import pallas as pl
from jax.experimental.pallas import tpu as pltpu
from jax.sharding import PartitionSpec as P

gas_gamma = 1.4
MESH = pl.DeviceIdType.MESH
BASE = 8
VEL, PRS, SND, LND, LNR, RAT = 5, 8, 9, 10, 11, 12
FIELDS = 13


def tables():
    inverse_root = 1.0 / math.sqrt(5.0)
    points = np.array([-1.0, -inverse_root, inverse_root, 1.0])
    weights = [1.0 / 6.0, 5.0 / 6.0, 5.0 / 6.0, 1.0 / 6.0]
    barycentric = np.array(
        [
            1.0 / np.prod([points[target] - points[other] for other in range(4) if other != target])
            for target in range(4)
        ]
    )
    derivative = np.zeros((4, 4))
    for target in range(4):
        for source in range(4):
            if target != source:
                derivative[target, source] = (
                    barycentric[source] / barycentric[target] / (points[target] - points[source])
                )
    legendre = np.stack(
        [np.ones(4), points, (3.0 * points**2 - 1.0) / 2.0, (5.0 * points**3 - 3.0 * points) / 2.0],
        1,
    )
    legendre = legendre * np.sqrt(np.arange(4) + 0.5)
    weight_column = np.array(weights)[:, None]
    discrete_norms = np.sum(weight_column * legendre * legendre, 0)
    inverse = (weight_column * legendre).T / discrete_norms[:, None]
    return (weights, derivative, inverse)


def mechanics(conserved):
    density, m1, m2, m3, energy = conserved
    inverse = 1.0 / density
    v1, v2, v3 = m1 * inverse, m2 * inverse, m3 * inverse
    pressure = (gas_gamma - 1.0) * (energy - 0.5 * density * (v1 * v1 + v2 * v2 + v3 * v3))
    sound = jnp.sqrt(gas_gamma * pressure * inverse)
    return [v1, v2, v3, pressure, sound]


def logarithms(density, pressure):
    ratio = density / pressure
    return [jnp.log(density), jnp.log(ratio), ratio]


def primitives(conserved):
    motion = mechanics(conserved)
    return list(conserved) + motion + logarithms(conserved[0], motion[3])


def mean_parts(a, b, log_a, log_b):
    total, gap = a + b, a - b
    relative = gap / total
    square = relative * relative
    small = square < 0.01
    series = 2.0 + square * (2.0 / 3.0 + square * (2.0 / 5.0 + square * (2.0 / 7.0)))
    return jnp.where(small, total, gap), jnp.where(small, series, log_a - log_b)


def entropy_flux(a, b, normal):
    num, den = mean_parts(a[0], b[0], a[LND], b[LND])
    mean_density = num / den
    num, den = mean_parts(a[RAT], b[RAT], a[LNR], b[LNR])
    inverse_beta = den / num
    velocity = [0.5 * (a[VEL + i] + b[VEL + i]) for i in range(3)]
    pressure = 0.5 * (a[PRS] + b[PRS])
    product = 0.5 * (a[5] * b[5] + a[6] * b[6] + a[7] * b[7])
    mass = mean_density * velocity[normal]
    out = [mass]
    for other in range(3):
        momentum = mass * velocity[other]
        out.append(momentum + pressure if other == normal else momentum)
    out.append(
        mass * (product + inverse_beta * (1.0 / (gas_gamma - 1.0)))
        + 0.5 * (a[PRS] * b[VEL + normal] + b[PRS] * a[VEL + normal])
    )
    return out


def dissipated(flux, a, b, normal):
    half = 0.5 * jnp.maximum(
        jnp.abs(a[VEL + normal]) + a[SND], jnp.abs(b[VEL + normal]) + b[SND]
    )
    return [flux[i] - half * (b[i] - a[i]) for i in range(5)]


def line_terms(nodes, normal, weights, deriv):
    vol = [[0.0] * 5 for _ in range(4)]
    diff = [[0.0] * 5 for _ in range(4)]
    for i in range(4):
        for j in range(i + 1, 4):
            flux = entropy_flux(nodes[i], nodes[j], normal)
            ci, cj = 2.0 * float(deriv[i, j]), 2.0 * float(deriv[j, i])
            if j == i + 1:
                face = dissipated(flux, nodes[i], nodes[j], normal)
            for f in range(5):
                vi, vj = ci * flux[f], cj * flux[f]
                vol[i][f] = vol[i][f] + vi
                vol[j][f] = vol[j][f] + vj
                if j == i + 1:
                    diff[i][f] = diff[i][f] + (face[f] * (1.0 / weights[i]) - vi)
                    diff[j][f] = diff[j][f] - (face[f] * (1.0 / weights[j]) + vj)
                else:
                    diff[i][f] = diff[i][f] - vi
                    diff[j][f] = diff[j][f] - vj
    return vol, diff


def make_kernel(ngx, ngy, nx, ny, nz):
    weights, deriv, inverse = tables()
    exl, eyl, rows = nx // 4, ny // 4, nx * ny
    total = ngx * ngy
    parts = 10 * (nx + ny) + 4 * exl * eyl
    roots = [(0, 0), (ngx - 1, 0), (1, 1), (1, 0)]
    group = 8 if (nx * eyl) % 8 == 0 else 4

    def kernel(u_in, inc, smooth_out, top_out, st, vol, dif, tq, ysend, yrecv, xrecv, yown, rb, rbr, near,
               bsc, mx, mx2, mxr, myr, span, sent, halo, tops, late):
        ix, iy = lax.axis_index("gx"), lax.axis_index("gy")
        loads = [pltpu.make_async_copy(u_in.at[f], st.at[f, BASE:BASE + rows], sent) for f in range(5)]
        for c in loads:
            c.start()
        barrier = pltpu.get_barrier_semaphore()
        rank = iy * ngx + ix
        is_root = [rank == y * ngx + x for x, y in roots]
        root = is_root[0]
        for here in is_root[1:]:
            root = jnp.logical_or(root, here)

        def greet(device):
            pl.semaphore_signal(barrier, 1, device_id=device, device_id_type=MESH)

        def visit(act):
            def step(k, carry):
                t = k + jnp.where(k >= rank, 1, 0)
                act({"gx": lax.rem(t, ngx), "gy": lax.div(t, ngx)})
                return carry

            lax.fori_loop(0, total - 1, step, 0)

        xup, xdn = {"gx": lax.rem(ix + 1, ngx)}, {"gx": lax.rem(ix + ngx - 1, ngx)}
        yup, ydn = {"gy": lax.rem(iy + 1, ngy)}, {"gy": lax.rem(iy + ngy - 1, ngy)}
        inner, wraps = iy > 0, iy == ngy - 1
        need = jnp.where(root, 6, 7) + jnp.where(inner, 1, 0)
        for device in (xup, xdn, ydn):
            greet(device)
        pl.when(jnp.logical_not(wraps))(lambda: greet(yup))

        @pl.when(root)
        def _():
            visit(greet)


        def remote(src, dst, rs, dev):
            return pltpu.make_async_remote_copy(
                src_ref=src, dst_ref=dst, send_sem=sent, recv_sem=rs, device_id=dev,
                device_id_type=MESH)

        def all_of(ref, count, sem):
            return remote(ref.at[0:count], ref.at[0:count], sem, xup)

        pltpu.make_async_copy(u_in, st.at[0:5, BASE:BASE + rows], sent).wait()
        top = None
        for r in range(0, rows, 8):
            density, m1, m2, m3, energy = [st[f, BASE + r:BASE + r + 8, :] for f in range(5)]
            unit = 1.0 / density
            v1, v2, v3 = m1 * unit, m2 * unit, m3 * unit
            inside = energy - 0.5 * density * (v1 * v1 + v2 * v2 + v3 * v3)
            sound = jnp.sqrt(gas_gamma * (gas_gamma - 1.0) * inside * unit)
            speed = jnp.abs(v1) + jnp.abs(v2) + jnp.abs(v3) + 3.0 * sound
            top = speed if top is None else jnp.maximum(top, speed)
        mx[...] = jnp.max(top, axis=0, keepdims=True)
        last = jnp.logical_and(wraps, ix >= ngx - 2)

        def meet():
            pl.semaphore_wait(barrier, need)

            for (x, y), here in zip(roots, is_root):
                @pl.when(jnp.logical_not(here))
                def _():
                    remote(mx, mxr.at[rank], tops, {"gx": x, "gy": y}).start()

        pl.when(last)(meet)
        lane = lax.broadcasted_iota(jnp.int32, (8, nz), 1)
        k = lane % 4
        k0, k1, k2, k3 = k == 0, k == 1, k == 2, k == 3

        def lanes(values):
            a, b, c, d = (float(v) for v in values)
            return jnp.where(k0, a, jnp.where(k1, b, jnp.where(k2, c, d))).astype(jnp.float32)

        def roll(x, s):
            return pltpu.roll(x, s % nz, 1)

        zcoef = {s: lanes([inverse[c, c + s] if 0 <= c + s < 4 else 0.0 for c in range(4)])
                 for s in range(-3, 4)}
        for r in range(0, rows, 8):
            here = slice(BASE + r, BASE + r + 8)
            p = mechanics([st[f, here, :] for f in range(5)])
            for f in range(5):
                st[VEL + f, here, :] = p[f]
            q = st[0, here, :] * p[3]
            t = zcoef[0] * q
            for s in (-3, -2, -1, 1, 2, 3):
                t = t + zcoef[s] * roll(q, -s)
            tq[r:r + 8, :] = t

        ke = k[:eyl]
        for e in range(exl):
            nodes = [[tq[pl.ds((4 * e + i) * ny + j, eyl, 4), :] for j in range(4)]
                     for i in range(4)]
            half = [[sum(float(inverse[a, i]) * nodes[i][j] for i in range(4))
                     for j in range(4)] for a in range(4)]
            e2 = e3 = e4 = 0.0
            for a in range(4):
                for b in range(4):
                    m = sum(float(inverse[b, j]) * half[a][j] for j in range(4))
                    m = m * m
                    e4 = e4 + m
                    if a < 3 and b < 3:
                        e3 = e3 + m
                    if a < 2 and b < 2:
                        e2 = e2 + m
            e3 = jnp.where(ke < 3, e3, 0.0)
            e2 = jnp.where(ke < 2, e2, 0.0)

            def spread(x):
                total = x
                for s in range(1, 4):
                    total = total + jnp.where(ke + s < 4, roll(x, -s), roll(x, 4 - s))
                return total

            e2, e3, e4 = spread(e2), spread(e3), spread(e4)
            energy = jnp.maximum((e4 - e3) / (e4 + 1e-06), (e3 - e2) / (e3 + 1e-06))
            threshold = 0.5 * 10.0 ** (-1.8 * 4.0**0.25)
            sharp = math.log(9999.0) / threshold
            raw = 1.0 / (1.0 + jnp.exp(-sharp * (energy - threshold)))
            raw = jnp.minimum(raw, 0.5)
            rb[e] = raw
        for f in range(5):
            ysend[0, f] = st[f, pl.ds(BASE + ny - 1, nx, ny), :]
            ysend[1, f] = st[f, pl.ds(BASE, nx, ny), :]
        mxr[rank] = mx[...]

        pl.when(jnp.logical_not(last))(meet)
        remote(ysend.at[0], yrecv.at[0], halo, yup).start()
        pl.when(inner)(lambda: remote(ysend.at[1], yrecv.at[1], halo, ydn).start())
        remote(st.at[0:5, BASE + rows - ny:BASE + rows], xrecv.at[0], halo, xup).start()
        remote(st.at[0:5, BASE:BASE + ny], xrecv.at[1], halo, xdn).start()
        remote(rb, rbr.at[2], halo, yup).start()
        pl.when(inner)(lambda: remote(rb, rbr.at[3], halo, ydn).start())
        remote(rb, rbr.at[0], halo, xup).start()
        remote(rb, rbr.at[1], halo, xdn).start()

        @pl.when(wraps)
        def _():
            pl.semaphore_signal(late, 1, device_id=yup, device_id_type=MESH)

        for r in range(0, rows, 8):
            here = slice(BASE + r, BASE + r + 8)
            p = logarithms(st[0, here, :], st[PRS, here, :])
            for f in range(3):
                st[LND + f, here, :] = p[f]
        for e in range(exl):
            raw = rb[e]
            close = jnp.maximum(roll(raw, 4), roll(raw, -4))
            if e > 0:
                close = jnp.maximum(close, rb[e - 1])
            if e < exl - 1:
                close = jnp.maximum(close, rb[e + 1])
            near[e, 8:8 + eyl, :] = raw
            near[e, 7:8, :] = raw[0:1]
            near[e, 8 + eyl:9 + eyl, :] = raw[eyl - 1:eyl]
            close = jnp.maximum(close, jnp.maximum(near[e, 7:7 + eyl, :], near[e, 9:9 + eyl, :]))
            bsc[e] = close

        ca = lanes([2 * deriv[0, 1], 2 * deriv[1, 2], 2 * deriv[2, 3], 1 / weights[3]])
        cb = lanes([2 * deriv[1, 0], 2 * deriv[2, 1], 2 * deriv[3, 2], -1 / weights[0]])
        da = lanes([1 / weights[0], 1 / weights[1], 1 / weights[2], 0.0])
        db = lanes([-1 / weights[1], -1 / weights[2], -1 / weights[3], 0.0])
        cam = jnp.where(k3, 0.0, ca)
        cbm = jnp.where(k3, 0.0, cb)
        mc = lanes([2 * deriv[0, 2], 2 * deriv[1, 3], 0.0, 2 * deriv[3, 0]])
        mr_ = lanes([2 * deriv[0, 3], 0.0, 2 * deriv[2, 0], 2 * deriv[3, 1]])

        def z_group(g, carry):
            row = g * 8
            own = [st[f, pl.ds(row + BASE, 8), :] for f in range(FIELDS)]
            nxt = [roll(x, -1) for x in own]
            far = [None] * FIELDS
            for f in (0, 5, 6, 7, PRS, LND, LNR, RAT):
                far[f] = jnp.where(k < 2, roll(own[f], -2), roll(own[f], 3))
            f1 = entropy_flux(own, nxt, 2)
            g1 = dissipated(f1, own, nxt, 2)
            fm = entropy_flux(own, far, 2)
            for f in range(5):
                sel = jnp.where(k3, g1[f], f1[f])
                mm = mc * fm[f] + mr_ * jnp.where(k0, roll(fm[f], -3), roll(fm[f], 2))
                vol[f, pl.ds(row, 8), :] = ca * sel + roll(cb * sel, 1) + mm
                dif[f, pl.ds(row, 8), :] = (
                    (da * g1[f] - cam * f1[f]) + roll(db * g1[f] - cbm * f1[f], 1) - mm)
            return carry

        for g in range(rows // 8):
            z_group(g, 0)

        for e in range(exl):
            for h in range(0, ny, 8):
                slabs = [(4 * e + i) * ny + h for i in range(4)]
                nodes = [[st[f, BASE + r:BASE + r + 8, :] for f in range(FIELDS)] for r in slabs]
                va, da_ = line_terms(nodes, 0, weights, deriv)
                for i in range(4):
                    for f in range(5):
                        vol[f, slabs[i]:slabs[i] + 8, :] += va[i][f]
                        dif[f, slabs[i]:slabs[i] + 8, :] += da_[i][f]
        for g in range(0, nx * eyl, group):
            def rows_of(ref, f, i, base):
                return ref[f, pl.ds(base + 4 * g + i, group, 4), :]

            nodes = [[rows_of(st, f, i, BASE) for f in range(FIELDS)] for i in range(4)]
            va, da_ = line_terms(nodes, 1, weights, deriv)
            for i in range(4):
                for f in range(5):
                    vol[f, pl.ds(4 * g + i, group, 4), :] += va[i][f]
                    dif[f, pl.ds(4 * g + i, group, 4), :] += da_[i][f]

        for e in range(1, exl):
            for h in range(0, ny, 8):
                r = 4 * e * ny + h
                a = [st[f, BASE + r - ny:BASE + r - ny + 8, :] for f in range(FIELDS)]
                b = [st[f, BASE + r:BASE + r + 8, :] for f in range(FIELDS)]
                face = dissipated(entropy_flux(a, b, 0), a, b, 0)
                for f in range(5):
                    vol[f, r - ny:r - ny + 8, :] += face[f] * (1.0 / weights[3])
                    vol[f, r:r + 8, :] -= face[f] * (1.0 / weights[0])
        for g in range(0, nx * eyl, group):
            ye = (lax.broadcasted_iota(jnp.int32, (group, nz), 0) + g) % eyl
            inside = ye < eyl - 1
            a = [st[f, pl.ds(BASE + 4 * g + 3, group, 4), :] for f in range(FIELDS)]
            b = [st[f, pl.ds(BASE + 4 * g + 4, group, 4), :] for f in range(FIELDS)]
            face = dissipated(entropy_flux(a, b, 1), a, b, 1)
            for f in range(5):
                kept = jnp.where(inside, face[f], 0.0)
                vol[f, pl.ds(4 * g + 3, group, 4), :] += kept * (1.0 / weights[3])
                vol[f, pl.ds(4 * g + 4, group, 4), :] -= kept * (1.0 / weights[0])
        for f in range(FIELDS):
            yown[f, 0:nx] = st[f, pl.ds(BASE, nx, ny), :]
            yown[f, nx:2 * nx] = st[f, pl.ds(BASE + ny - 1, nx, ny), :]

        @pl.when(jnp.logical_not(inner))
        def _():
            pl.semaphore_wait(late, 1)
            remote(ysend.at[1], yrecv.at[1], halo, ydn).start()
            remote(rb, rbr.at[3], halo, ydn).start()

        all_of(span, parts, halo).wait_recv()
        for h in range(0, ny, 8):
            for side in range(2):
                got = primitives([xrecv[side, f, h:h + 8, :] for f in range(5)])
                r = h if side == 0 else rows - ny + h
                own = [st[f, BASE + r:BASE + r + 8, :] for f in range(FIELDS)]
                a, b = (got, own) if side == 0 else (own, got)
                face = dissipated(entropy_flux(a, b, 0), a, b, 0)
                scale = -1.0 / weights[0] if side == 0 else 1.0 / weights[3]
                for f in range(5):
                    vol[f, r:r + 8, :] += face[f] * scale

        row = lax.broadcasted_iota(jnp.int32, (eyl, nz), 0)
        pick = (lax.broadcasted_iota(jnp.int32, (nz, nz // 4), 0)
                == 4 * lax.broadcasted_iota(jnp.int32, (nz, nz // 4), 1)).astype(jnp.float32)
        for e in range(exl):
            close = bsc[e]
            if e == 0:
                close = jnp.maximum(close, rbr[0, exl - 1])
            if e == exl - 1:
                close = jnp.maximum(close, rbr[1, 0])
            close = jnp.maximum(close, jnp.where(row == 0, rbr[2, e, eyl - 1:eyl, :], 0.0))
            close = jnp.maximum(close, jnp.where(row == eyl - 1, rbr[3, e, 0:1, :], 0.0))
            smooth = jnp.maximum(rb[e], 0.5 * close)
            bsc[e] = smooth
            smooth_out[e] = jnp.dot(smooth, pick, precision=lax.Precision.HIGHEST,
                                    preferred_element_type=jnp.float32)

        got = primitives([jnp.concatenate([yrecv[0, f], yrecv[1, f]], axis=0) for f in range(5)])
        own = [yown[f] for f in range(FIELDS)]
        first = lax.broadcasted_iota(jnp.int32, (2 * nx, nz), 0) < nx
        a = [jnp.where(first, got[f], own[f]) for f in range(FIELDS)]
        b = [jnp.where(first, own[f], got[f]) for f in range(FIELDS)]
        face = dissipated(entropy_flux(a, b, 1), a, b, 1)
        for f in range(5):
            vol[f, pl.ds(0, nx, ny), :] -= face[f][:nx] * (1.0 / weights[0])
            vol[f, pl.ds(ny - 1, nx, ny), :] += face[f][nx:] * (1.0 / weights[3])
        under = lax.broadcasted_iota(jnp.int32, (8, nz), 0) < 4
        for e in range(exl):
            for h in range(0, ny, 8):
                y = h // 4
                b = jnp.where(under, bsc[e, y:y + 1, :], bsc[e, y + 1:y + 2, :])
                for i in range(4):
                    r = (4 * e + i) * ny + h
                    for f in range(5):
                        inc[f, r:r + 8, :] = vol[f, r:r + 8, :] + b * dif[f, r:r + 8, :]
        for here, count in ((root, 3), (jnp.logical_not(root), 4)):
            @pl.when(here)
            def _():
                all_of(span, parts + count, tops).wait_send()

        def gather():
            all_of(mxr, total - 1, tops).wait_recv()
            found = [mxr[i] for i in range(total)]
            while len(found) > 1:
                pairs = [jnp.maximum(a, b) for a, b in zip(found[::2], found[1::2])]
                found = pairs + found[2 * len(pairs):]
            return found[0]

        for hub, mine in ((1, lambda x, odd: x >= 2 or not odd), (2, lambda x, odd: x < 2 and odd)):
            @pl.when(is_root[hub])
            def _():
                mx2[...] = gather()

                def send(h, carry):
                    for odd in range(2):
                        for x in range(ngx):
                            if mine(x, odd) and not (isinstance(h, int) and (x, 2 * h + odd) in roots):
                                remote(mx2, myr, tops, {"gx": x, "gy": 2 * h + odd}).start()
                    return carry

                for h in range(min(ngy // 2, 16)):
                    send(h, 0)
                if ngy > 32:
                    lax.fori_loop(16, ngy // 2, send, 0)
                top_out[...] = mx2[...]
                count = sum(mine(x, y % 2) and (x, y) not in roots
                            for x in range(ngx) for y in range(ngy))
                all_of(mxr, count, tops).wait_send()

        @pl.when(jnp.logical_not(root))
        def _():
            remote(mx2, myr, tops, xup).wait_recv()
            top_out[...] = myr[...]

        @pl.when(jnp.logical_or(is_root[0], is_root[3]))
        def _():
            top_out[...] = gather()

    f32 = jnp.float32
    dma = pltpu.SemaphoreType.DMA
    pad = BASE + rows + 8
    scratch = [
        pltpu.VMEM((FIELDS, pad, nz), f32),
        pltpu.VMEM((5, rows + 8, nz), f32),
        pltpu.VMEM((5, rows, nz), f32),
        pltpu.VMEM((rows, nz), f32),
        pltpu.VMEM((2, 5, nx, nz), f32),
        pltpu.VMEM((2, 5, nx, nz), f32),
        pltpu.VMEM((2, 5, ny, nz), f32),
        pltpu.VMEM((FIELDS, 2 * nx, nz), f32),
        pltpu.VMEM((exl, eyl, nz), f32),
        pltpu.VMEM((4, exl, eyl, nz), f32),
        pltpu.VMEM((exl, eyl + 16, nz), f32),
        pltpu.VMEM((exl, eyl, nz), f32),
        pltpu.VMEM((1, nz), f32),
        pltpu.VMEM((1, nz), f32),
        pltpu.VMEM((total, 1, nz), f32),
        pltpu.VMEM((1, nz), f32),
        pltpu.VMEM((parts + 4, 1, nz), f32),
        dma, dma, dma,
        pltpu.SemaphoreType.REGULAR,
    ]
    return kernel, scratch


def finish(raw, smooth, top, inc, bl, scaled, done):
    blend = pltpu.make_async_copy(smooth, bl, done)
    blend.start()
    peak = jnp.broadcast_to(top[...], (8, top.shape[1]))
    step = -0.25 / jnp.max(peak, axis=1, keepdims=True)
    rows = raw.shape[1]
    half = max(rows // 16 * 8, 8)
    for f in range(5):
        for low in range(0, rows, half):
            high = min(low + half, rows)
            for r in range(low, high, 8):
                scaled[f, r:r + 8, :] = step * raw[f, r:r + 8, :]
            pltpu.make_async_copy(scaled.at[f, low:high], inc.at[f, low:high], done).start()
    pltpu.make_async_copy(scaled, inc, done).wait()
    blend.wait()


def solution(mesh):
    ngx, ngy = mesh.shape["gx"], mesh.shape["gy"]

    def body(conserved):
        _, nx, ny, nz = conserved.shape
        kernel, scratch = make_kernel(ngx, ngy, nx, ny, nz)
        vmem = pl.BlockSpec(memory_space=pltpu.VMEM)
        shape = lambda *dims: jax.ShapeDtypeStruct(dims, jnp.float32)
        raw, smooth, top = pl.pallas_call(
            kernel,
            out_shape=(shape(5, nx * ny, nz), shape(nx // 4, ny // 4, nz // 4), shape(1, nz)),
            in_specs=[pl.BlockSpec(memory_space=pltpu.HBM)],
            out_specs=(vmem, vmem, vmem),
            scratch_shapes=scratch,
            compiler_params=pltpu.CompilerParams(
                collective_id=0, has_side_effects=True, vmem_limit_bytes=12 * 2**20),
            name="section",
        )(pltpu.with_memory_space_constraint(
            conserved.reshape(5, nx * ny, nz), pltpu.HBM))
        inc, blending = pl.pallas_call(
            finish,
            out_shape=(shape(5, nx * ny, nz), shape(nx // 4, ny // 4, nz // 4)),
            in_specs=[vmem, vmem, vmem],
            out_specs=(pl.BlockSpec(memory_space=pltpu.HBM),) * 2,
            scratch_shapes=[pltpu.VMEM((5, nx * ny, nz), jnp.float32), pltpu.SemaphoreType.DMA],
            compiler_params=pltpu.CompilerParams(vmem_limit_bytes=8 * 2**20),
            name="finish",
        )(raw, smooth, top)
        return inc.reshape(conserved.shape), blending

    return jax.shard_map(
        body, mesh=mesh, in_specs=(P(None, "gx", "gy", None),),
        out_specs=(P(None, "gx", "gy", None), P("gx", "gy", None)), check_vma=False)
```

```python
import math

import jax
import jax.numpy as jnp
import numpy as np
from jax import lax
from jax.experimental import pallas as pl
from jax.experimental.pallas import tpu as pltpu
from jax.sharding import PartitionSpec as P

gas_gamma = 1.4
MESH = pl.DeviceIdType.MESH
BASE = 8
VEL, PRS, SND, LND, LNR, RAT = 5, 8, 9, 10, 11, 12
FIELDS = 13


def tables():
    inverse_root = 1.0 / math.sqrt(5.0)
    points = np.array([-1.0, -inverse_root, inverse_root, 1.0])
    weights = [1.0 / 6.0, 5.0 / 6.0, 5.0 / 6.0, 1.0 / 6.0]
    barycentric = np.array(
        [
            1.0 / np.prod([points[target] - points[other] for other in range(4) if other != target])
            for target in range(4)
        ]
    )
    derivative = np.zeros((4, 4))
    for target in range(4):
        for source in range(4):
            if target != source:
                derivative[target, source] = (
                    barycentric[source] / barycentric[target] / (points[target] - points[source])
                )
    legendre = np.stack(
        [np.ones(4), points, (3.0 * points**2 - 1.0) / 2.0, (5.0 * points**3 - 3.0 * points) / 2.0],
        1,
    )
    legendre = legendre * np.sqrt(np.arange(4) + 0.5)
    weight_column = np.array(weights)[:, None]
    discrete_norms = np.sum(weight_column * legendre * legendre, 0)
    inverse = (weight_column * legendre).T / discrete_norms[:, None]
    return (weights, derivative, inverse)


def mechanics(conserved):
    density, m1, m2, m3, energy = conserved
    inverse = 1.0 / density
    v1, v2, v3 = m1 * inverse, m2 * inverse, m3 * inverse
    pressure = (gas_gamma - 1.0) * (energy - 0.5 * density * (v1 * v1 + v2 * v2 + v3 * v3))
    sound = jnp.sqrt(gas_gamma * pressure * inverse)
    return [v1, v2, v3, pressure, sound]


def logarithms(density, pressure):
    ratio = density / pressure
    return [jnp.log(density), jnp.log(ratio), ratio]


def primitives(conserved):
    motion = mechanics(conserved)
    return list(conserved) + motion + logarithms(conserved[0], motion[3])


def mean_parts(a, b, log_a, log_b):
    total, gap = a + b, a - b
    relative = gap / total
    square = relative * relative
    small = square < 0.01
    series = 2.0 + square * (2.0 / 3.0 + square * (2.0 / 5.0 + square * (2.0 / 7.0)))
    return jnp.where(small, total, gap), jnp.where(small, series, log_a - log_b)


def entropy_flux(a, b, normal):
    num, den = mean_parts(a[0], b[0], a[LND], b[LND])
    mean_density = num / den
    num, den = mean_parts(a[RAT], b[RAT], a[LNR], b[LNR])
    inverse_beta = den / num
    velocity = [0.5 * (a[VEL + i] + b[VEL + i]) for i in range(3)]
    pressure = 0.5 * (a[PRS] + b[PRS])
    product = 0.5 * (a[5] * b[5] + a[6] * b[6] + a[7] * b[7])
    mass = mean_density * velocity[normal]
    out = [mass]
    for other in range(3):
        momentum = mass * velocity[other]
        out.append(momentum + pressure if other == normal else momentum)
    out.append(
        mass * (product + inverse_beta * (1.0 / (gas_gamma - 1.0)))
        + 0.5 * (a[PRS] * b[VEL + normal] + b[PRS] * a[VEL + normal])
    )
    return out


def dissipated(flux, a, b, normal):
    half = 0.5 * jnp.maximum(
        jnp.abs(a[VEL + normal]) + a[SND], jnp.abs(b[VEL + normal]) + b[SND]
    )
    return [flux[i] - half * (b[i] - a[i]) for i in range(5)]


def line_terms(nodes, normal, weights, deriv):
    vol = [[0.0] * 5 for _ in range(4)]
    diff = [[0.0] * 5 for _ in range(4)]
    for i in range(4):
        for j in range(i + 1, 4):
            flux = entropy_flux(nodes[i], nodes[j], normal)
            ci, cj = 2.0 * float(deriv[i, j]), 2.0 * float(deriv[j, i])
            if j == i + 1:
                face = dissipated(flux, nodes[i], nodes[j], normal)
            for f in range(5):
                vi, vj = ci * flux[f], cj * flux[f]
                vol[i][f] = vol[i][f] + vi
                vol[j][f] = vol[j][f] + vj
                if j == i + 1:
                    diff[i][f] = diff[i][f] + (face[f] * (1.0 / weights[i]) - vi)
                    diff[j][f] = diff[j][f] - (face[f] * (1.0 / weights[j]) + vj)
                else:
                    diff[i][f] = diff[i][f] - vi
                    diff[j][f] = diff[j][f] - vj
    return vol, diff


def make_kernel(ngx, ngy, nx, ny, nz):
    weights, deriv, inverse = tables()
    exl, eyl, rows = nx // 4, ny // 4, nx * ny
    total = ngx * ngy
    parts = 10 * (nx + ny) + 4 * exl * eyl
    roots = [(0, 0), (ngx - 1, 0), (1, 1), (1, 0)]
    group = 8 if (nx * eyl) % 8 == 0 else 4

    def kernel(u_in, inc, smooth_out, top_out, st, vol, dif, tq, ysend, yrecv, xrecv, yown, rb, rbr, near,
               bsc, mx, mx2, mxr, myr, span, sent, halo, tops, late):
        ix, iy = lax.axis_index("gx"), lax.axis_index("gy")
        loads = [pltpu.make_async_copy(u_in.at[f], st.at[f, BASE:BASE + rows], sent) for f in range(5)]
        for c in loads:
            c.start()
        barrier = pltpu.get_barrier_semaphore()
        rank = iy * ngx + ix
        is_root = [rank == y * ngx + x for x, y in roots]
        root = is_root[0]
        for here in is_root[1:]:
            root = jnp.logical_or(root, here)

        def greet(device):
            pl.semaphore_signal(barrier, 1, device_id=device, device_id_type=MESH)

        def visit(act):
            def step(k, carry):
                t = k + jnp.where(k >= rank, 1, 0)
                act({"gx": lax.rem(t, ngx), "gy": lax.div(t, ngx)})
                return carry

            lax.fori_loop(0, total - 1, step, 0)

        xup, xdn = {"gx": lax.rem(ix + 1, ngx)}, {"gx": lax.rem(ix + ngx - 1, ngx)}
        yup, ydn = {"gy": lax.rem(iy + 1, ngy)}, {"gy": lax.rem(iy + ngy - 1, ngy)}
        inner, wraps = iy > 0, iy == ngy - 1
        need = jnp.where(root, 6, 7) + jnp.where(inner, 1, 0)
        for device in (xup, xdn, ydn):
            greet(device)
        pl.when(jnp.logical_not(wraps))(lambda: greet(yup))

        @pl.when(root)
        def _():
            visit(greet)


        def remote(src, dst, rs, dev):
            return pltpu.make_async_remote_copy(
                src_ref=src, dst_ref=dst, send_sem=sent, recv_sem=rs, device_id=dev,
                device_id_type=MESH)

        def all_of(ref, count, sem):
            return remote(ref.at[0:count], ref.at[0:count], sem, xup)

        pltpu.make_async_copy(u_in, st.at[0:5, BASE:BASE + rows], sent).wait()
        top = None
        for r in range(0, rows, 8):
            density, m1, m2, m3, energy = [st[f, BASE + r:BASE + r + 8, :] for f in range(5)]
            unit = 1.0 / density
            v1, v2, v3 = m1 * unit, m2 * unit, m3 * unit
            inside = energy - 0.5 * density * (v1 * v1 + v2 * v2 + v3 * v3)
            sound = jnp.sqrt(gas_gamma * (gas_gamma - 1.0) * inside * unit)
            speed = jnp.abs(v1) + jnp.abs(v2) + jnp.abs(v3) + 3.0 * sound
            top = speed if top is None else jnp.maximum(top, speed)
        mx[...] = jnp.max(top, axis=0, keepdims=True)
        last = jnp.logical_and(wraps, ix >= ngx - 2)

        def meet():
            pl.semaphore_wait(barrier, need)

            for (x, y), here in zip(roots, is_root):
                @pl.when(jnp.logical_not(here))
                def _():
                    remote(mx, mxr.at[rank], tops, {"gx": x, "gy": y}).start()

        pl.when(last)(meet)
        lane = lax.broadcasted_iota(jnp.int32, (8, nz), 1)
        k = lane % 4
        k0, k1, k2, k3 = k == 0, k == 1, k == 2, k == 3

        def lanes(values):
            a, b, c, d = (float(v) for v in values)
            return jnp.where(k0, a, jnp.where(k1, b, jnp.where(k2, c, d))).astype(jnp.float32)

        def roll(x, s):
            return pltpu.roll(x, s % nz, 1)

        zcoef = {s: lanes([inverse[c, c + s] if 0 <= c + s < 4 else 0.0 for c in range(4)])
                 for s in range(-3, 4)}
        for r in range(0, rows, 8):
            here = slice(BASE + r, BASE + r + 8)
            p = mechanics([st[f, here, :] for f in range(5)])
            for f in range(5):
                st[VEL + f, here, :] = p[f]
            q = st[0, here, :] * p[3]
            t = zcoef[0] * q
            for s in (-3, -2, -1, 1, 2, 3):
                t = t + zcoef[s] * roll(q, -s)
            tq[r:r + 8, :] = t

        ke = k[:eyl]
        for e in range(exl):
            nodes = [[tq[pl.ds((4 * e + i) * ny + j, eyl, 4), :] for j in range(4)]
                     for i in range(4)]
            half = [[sum(float(inverse[a, i]) * nodes[i][j] for i in range(4))
                     for j in range(4)] for a in range(4)]
            e2 = e3 = e4 = 0.0
            for a in range(4):
                for b in range(4):
                    m = sum(float(inverse[b, j]) * half[a][j] for j in range(4))
                    m = m * m
                    e4 = e4 + m
                    if a < 3 and b < 3:
                        e3 = e3 + m
                    if a < 2 and b < 2:
                        e2 = e2 + m
            e3 = jnp.where(ke < 3, e3, 0.0)
            e2 = jnp.where(ke < 2, e2, 0.0)

            def spread(x):
                total = x
                for s in range(1, 4):
                    total = total + jnp.where(ke + s < 4, roll(x, -s), roll(x, 4 - s))
                return total

            e2, e3, e4 = spread(e2), spread(e3), spread(e4)
            energy = jnp.maximum((e4 - e3) / (e4 + 1e-06), (e3 - e2) / (e3 + 1e-06))
            threshold = 0.5 * 10.0 ** (-1.8 * 4.0**0.25)
            sharp = math.log(9999.0) / threshold
            raw = 1.0 / (1.0 + jnp.exp(-sharp * (energy - threshold)))
            raw = jnp.minimum(raw, 0.5)
            rb[e] = raw
        for f in range(5):
            ysend[0, f] = st[f, pl.ds(BASE + ny - 1, nx, ny), :]
            ysend[1, f] = st[f, pl.ds(BASE, nx, ny), :]
        mxr[rank] = mx[...]

        pl.when(jnp.logical_not(last))(meet)
        remote(ysend.at[0], yrecv.at[0], halo, yup).start()
        pl.when(inner)(lambda: remote(ysend.at[1], yrecv.at[1], halo, ydn).start())
        remote(st.at[0:5, BASE + rows - ny:BASE + rows], xrecv.at[0], halo, xup).start()
        remote(st.at[0:5, BASE:BASE + ny], xrecv.at[1], halo, xdn).start()
        remote(rb, rbr.at[2], halo, yup).start()
        pl.when(inner)(lambda: remote(rb, rbr.at[3], halo, ydn).start())
        remote(rb, rbr.at[0], halo, xup).start()
        remote(rb, rbr.at[1], halo, xdn).start()

        @pl.when(wraps)
        def _():
            pl.semaphore_signal(late, 1, device_id=yup, device_id_type=MESH)

        for r in range(0, rows, 8):
            here = slice(BASE + r, BASE + r + 8)
            p = logarithms(st[0, here, :], st[PRS, here, :])
            for f in range(3):
                st[LND + f, here, :] = p[f]
        for e in range(exl):
            raw = rb[e]
            close = jnp.maximum(roll(raw, 4), roll(raw, -4))
            if e > 0:
                close = jnp.maximum(close, rb[e - 1])
            if e < exl - 1:
                close = jnp.maximum(close, rb[e + 1])
            near[e, 8:8 + eyl, :] = raw
            near[e, 7:8, :] = raw[0:1]
            near[e, 8 + eyl:9 + eyl, :] = raw[eyl - 1:eyl]
            close = jnp.maximum(close, jnp.maximum(near[e, 7:7 + eyl, :], near[e, 9:9 + eyl, :]))
            bsc[e] = close

        ca = lanes([2 * deriv[0, 1], 2 * deriv[1, 2], 2 * deriv[2, 3], 1 / weights[3]])
        cb = lanes([2 * deriv[1, 0], 2 * deriv[2, 1], 2 * deriv[3, 2], -1 / weights[0]])
        da = lanes([1 / weights[0], 1 / weights[1], 1 / weights[2], 0.0])
        db = lanes([-1 / weights[1], -1 / weights[2], -1 / weights[3], 0.0])
        cam = jnp.where(k3, 0.0, ca)
        cbm = jnp.where(k3, 0.0, cb)
        mc = lanes([2 * deriv[0, 2], 2 * deriv[1, 3], 0.0, 2 * deriv[3, 0]])
        mr_ = lanes([2 * deriv[0, 3], 0.0, 2 * deriv[2, 0], 2 * deriv[3, 1]])

        def z_group(g, carry):
            row = pl.multiple_of(g * 8, 8)
            own = [st[f, pl.ds(row + BASE, 8), :] for f in range(FIELDS)]
            nxt = [roll(x, -1) for x in own]
            far = [None] * FIELDS
            for f in (0, 5, 6, 7, PRS, LND, LNR, RAT):
                far[f] = jnp.where(k < 2, roll(own[f], -2), roll(own[f], 3))
            f1 = entropy_flux(own, nxt, 2)
            g1 = dissipated(f1, own, nxt, 2)
            fm = entropy_flux(own, far, 2)
            for f in range(5):
                sel = jnp.where(k3, g1[f], f1[f])
                mm = mc * fm[f] + mr_ * jnp.where(k0, roll(fm[f], -3), roll(fm[f], 2))
                vol[f, pl.ds(row, 8), :] = ca * sel + roll(cb * sel, 1) + mm
                dif[f, pl.ds(row, 8), :] = (
                    (da * g1[f] - cam * f1[f]) + roll(db * g1[f] - cbm * f1[f], 1) - mm)
            return carry

        lax.fori_loop(0, rows // 8, z_group, 0)

        for e in range(exl):
            for h in range(0, ny, 8):
                slabs = [(4 * e + i) * ny + h for i in range(4)]
                nodes = [[st[f, BASE + r:BASE + r + 8, :] for f in range(FIELDS)] for r in slabs]
                va, da_ = line_terms(nodes, 0, weights, deriv)
                for i in range(4):
                    for f in range(5):
                        vol[f, slabs[i]:slabs[i] + 8, :] += va[i][f]
                        dif[f, slabs[i]:slabs[i] + 8, :] += da_[i][f]
        for g in range(0, nx * eyl, group):
            def rows_of(ref, f, i, base):
                return ref[f, pl.ds(base + 4 * g + i, group, 4), :]

            nodes = [[rows_of(st, f, i, BASE) for f in range(FIELDS)] for i in range(4)]
            va, da_ = line_terms(nodes, 1, weights, deriv)
            for i in range(4):
                for f in range(5):
                    vol[f, pl.ds(4 * g + i, group, 4), :] += va[i][f]
                    dif[f, pl.ds(4 * g + i, group, 4), :] += da_[i][f]

        for e in range(1, exl):
            for h in range(0, ny, 8):
                r = 4 * e * ny + h
                a = [st[f, BASE + r - ny:BASE + r - ny + 8, :] for f in range(FIELDS)]
                b = [st[f, BASE + r:BASE + r + 8, :] for f in range(FIELDS)]
                face = dissipated(entropy_flux(a, b, 0), a, b, 0)
                for f in range(5):
                    vol[f, r - ny:r - ny + 8, :] += face[f] * (1.0 / weights[3])
                    vol[f, r:r + 8, :] -= face[f] * (1.0 / weights[0])
        for g in range(0, nx * eyl, group):
            ye = (lax.broadcasted_iota(jnp.int32, (group, nz), 0) + g) % eyl
            inside = ye < eyl - 1
            a = [st[f, pl.ds(BASE + 4 * g + 3, group, 4), :] for f in range(FIELDS)]
            b = [st[f, pl.ds(BASE + 4 * g + 4, group, 4), :] for f in range(FIELDS)]
            face = dissipated(entropy_flux(a, b, 1), a, b, 1)
            for f in range(5):
                kept = jnp.where(inside, face[f], 0.0)
                vol[f, pl.ds(4 * g + 3, group, 4), :] += kept * (1.0 / weights[3])
                vol[f, pl.ds(4 * g + 4, group, 4), :] -= kept * (1.0 / weights[0])
        for f in range(FIELDS):
            yown[f, 0:nx] = st[f, pl.ds(BASE, nx, ny), :]
            yown[f, nx:2 * nx] = st[f, pl.ds(BASE + ny - 1, nx, ny), :]

        @pl.when(jnp.logical_not(inner))
        def _():
            pl.semaphore_wait(late, 1)
            remote(ysend.at[1], yrecv.at[1], halo, ydn).start()
            remote(rb, rbr.at[3], halo, ydn).start()

        all_of(span, parts, halo).wait_recv()
        for h in range(0, ny, 8):
            for side in range(2):
                got = primitives([xrecv[side, f, h:h + 8, :] for f in range(5)])
                r = h if side == 0 else rows - ny + h
                own = [st[f, BASE + r:BASE + r + 8, :] for f in range(FIELDS)]
                a, b = (got, own) if side == 0 else (own, got)
                face = dissipated(entropy_flux(a, b, 0), a, b, 0)
                scale = -1.0 / weights[0] if side == 0 else 1.0 / weights[3]
                for f in range(5):
                    vol[f, r:r + 8, :] += face[f] * scale

        row = lax.broadcasted_iota(jnp.int32, (eyl, nz), 0)
        pick = (lax.broadcasted_iota(jnp.int32, (nz, nz // 4), 0)
                == 4 * lax.broadcasted_iota(jnp.int32, (nz, nz // 4), 1)).astype(jnp.float32)
        for e in range(exl):
            close = bsc[e]
            if e == 0:
                close = jnp.maximum(close, rbr[0, exl - 1])
            if e == exl - 1:
                close = jnp.maximum(close, rbr[1, 0])
            close = jnp.maximum(close, jnp.where(row == 0, rbr[2, e, eyl - 1:eyl, :], 0.0))
            close = jnp.maximum(close, jnp.where(row == eyl - 1, rbr[3, e, 0:1, :], 0.0))
            smooth = jnp.maximum(rb[e], 0.5 * close)
            bsc[e] = smooth
            smooth_out[e] = jnp.dot(smooth, pick, precision=lax.Precision.HIGHEST,
                                    preferred_element_type=jnp.float32)

        got = primitives([jnp.concatenate([yrecv[0, f], yrecv[1, f]], axis=0) for f in range(5)])
        own = [yown[f] for f in range(FIELDS)]
        first = lax.broadcasted_iota(jnp.int32, (2 * nx, nz), 0) < nx
        a = [jnp.where(first, got[f], own[f]) for f in range(FIELDS)]
        b = [jnp.where(first, own[f], got[f]) for f in range(FIELDS)]
        face = dissipated(entropy_flux(a, b, 1), a, b, 1)
        for f in range(5):
            vol[f, pl.ds(0, nx, ny), :] -= face[f][:nx] * (1.0 / weights[0])
            vol[f, pl.ds(ny - 1, nx, ny), :] += face[f][nx:] * (1.0 / weights[3])
        under = lax.broadcasted_iota(jnp.int32, (8, nz), 0) < 4
        for e in range(exl):
            for h in range(0, ny, 8):
                y = h // 4
                b = jnp.where(under, bsc[e, y:y + 1, :], bsc[e, y + 1:y + 2, :])
                for i in range(4):
                    r = (4 * e + i) * ny + h
                    for f in range(5):
                        inc[f, r:r + 8, :] = vol[f, r:r + 8, :] + b * dif[f, r:r + 8, :]
        for here, count in ((root, 3), (jnp.logical_not(root), 4)):
            @pl.when(here)
            def _():
                all_of(span, parts + count, tops).wait_send()

        def gather():
            all_of(mxr, total - 1, tops).wait_recv()
            found = [mxr[i] for i in range(total)]
            while len(found) > 1:
                pairs = [jnp.maximum(a, b) for a, b in zip(found[::2], found[1::2])]
                found = pairs + found[2 * len(pairs):]
            return found[0]

        for hub, mine in ((1, lambda x, odd: x >= 2 or not odd), (2, lambda x, odd: x < 2 and odd)):
            @pl.when(is_root[hub])
            def _():
                mx2[...] = gather()

                def send(h, carry):
                    for odd in range(2):
                        for x in range(ngx):
                            if mine(x, odd) and not (isinstance(h, int) and (x, 2 * h + odd) in roots):
                                remote(mx2, myr, tops, {"gx": x, "gy": 2 * h + odd}).start()
                    return carry

                for h in range(min(ngy // 2, 16)):
                    send(h, 0)
                if ngy > 32:
                    lax.fori_loop(16, ngy // 2, send, 0)
                top_out[...] = mx2[...]
                count = sum(mine(x, y % 2) and (x, y) not in roots
                            for x in range(ngx) for y in range(ngy))
                all_of(mxr, count, tops).wait_send()

        @pl.when(jnp.logical_not(root))
        def _():
            remote(mx2, myr, tops, xup).wait_recv()
            top_out[...] = myr[...]

        @pl.when(jnp.logical_or(is_root[0], is_root[3]))
        def _():
            top_out[...] = gather()

    f32 = jnp.float32
    dma = pltpu.SemaphoreType.DMA
    pad = BASE + rows + 8
    scratch = [
        pltpu.VMEM((FIELDS, pad, nz), f32),
        pltpu.VMEM((5, rows + 8, nz), f32),
        pltpu.VMEM((5, rows, nz), f32),
        pltpu.VMEM((rows, nz), f32),
        pltpu.VMEM((2, 5, nx, nz), f32),
        pltpu.VMEM((2, 5, nx, nz), f32),
        pltpu.VMEM((2, 5, ny, nz), f32),
        pltpu.VMEM((FIELDS, 2 * nx, nz), f32),
        pltpu.VMEM((exl, eyl, nz), f32),
        pltpu.VMEM((4, exl, eyl, nz), f32),
        pltpu.VMEM((exl, eyl + 16, nz), f32),
        pltpu.VMEM((exl, eyl, nz), f32),
        pltpu.VMEM((1, nz), f32),
        pltpu.VMEM((1, nz), f32),
        pltpu.VMEM((total, 1, nz), f32),
        pltpu.VMEM((1, nz), f32),
        pltpu.VMEM((parts + 4, 1, nz), f32),
        dma, dma, dma,
        pltpu.SemaphoreType.REGULAR,
    ]
    return kernel, scratch


def finish(raw, smooth, top, inc, bl, scaled, done):
    blend = pltpu.make_async_copy(smooth, bl, done)
    blend.start()
    peak = jnp.broadcast_to(top[...], (8, top.shape[1]))
    step = -0.25 / jnp.max(peak, axis=1, keepdims=True)
    rows = raw.shape[1]
    half = max(rows // 16 * 8, 8)
    for f in range(5):
        for low in range(0, rows, half):
            high = min(low + half, rows)
            for r in range(low, high, 8):
                scaled[f, r:r + 8, :] = step * raw[f, r:r + 8, :]
            pltpu.make_async_copy(scaled.at[f, low:high], inc.at[f, low:high], done).start()
    pltpu.make_async_copy(scaled, inc, done).wait()
    blend.wait()


def solution(mesh):
    ngx, ngy = mesh.shape["gx"], mesh.shape["gy"]

    def body(conserved):
        _, nx, ny, nz = conserved.shape
        kernel, scratch = make_kernel(ngx, ngy, nx, ny, nz)
        vmem = pl.BlockSpec(memory_space=pltpu.VMEM)
        shape = lambda *dims: jax.ShapeDtypeStruct(dims, jnp.float32)
        raw, smooth, top = pl.pallas_call(
            kernel,
            out_shape=(shape(5, nx * ny, nz), shape(nx // 4, ny // 4, nz // 4), shape(1, nz)),
            in_specs=[pl.BlockSpec(memory_space=pltpu.HBM)],
            out_specs=(vmem, vmem, vmem),
            scratch_shapes=scratch,
            compiler_params=pltpu.CompilerParams(
                collective_id=0, has_side_effects=True, vmem_limit_bytes=12 * 2**20),
            name="section",
        )(pltpu.with_memory_space_constraint(
            conserved.reshape(5, nx * ny, nz), pltpu.HBM))
        inc, blending = pl.pallas_call(
            finish,
            out_shape=(shape(5, nx * ny, nz), shape(nx // 4, ny // 4, nz // 4)),
            in_specs=[vmem, vmem, vmem],
            out_specs=(pl.BlockSpec(memory_space=pltpu.HBM),) * 2,
            scratch_shapes=[pltpu.VMEM((5, nx * ny, nz), jnp.float32), pltpu.SemaphoreType.DMA],
            compiler_params=pltpu.CompilerParams(vmem_limit_bytes=8 * 2**20),
            name="finish",
        )(raw, smooth, top)
        return inc.reshape(conserved.shape), blending

    return jax.shard_map(
        body, mesh=mesh, in_specs=(P(None, "gx", "gy", None),),
        out_specs=(P(None, "gx", "gy", None), P("gx", "gy", None)), check_vma=False)
```

```python
import math

import jax
import jax.numpy as jnp
import numpy as np
from jax import lax
from jax.experimental import pallas as pl
from jax.experimental.pallas import tpu as pltpu
from jax.sharding import PartitionSpec as P

gas_gamma = 1.4
MESH = pl.DeviceIdType.MESH
BASE = 8
VEL, PRS, SND, LND, LNR, RAT = 5, 8, 9, 10, 11, 12
FIELDS = 13


def tables():
    inverse_root = 1.0 / math.sqrt(5.0)
    points = np.array([-1.0, -inverse_root, inverse_root, 1.0])
    weights = [1.0 / 6.0, 5.0 / 6.0, 5.0 / 6.0, 1.0 / 6.0]
    barycentric = np.array(
        [
            1.0 / np.prod([points[target] - points[other] for other in range(4) if other != target])
            for target in range(4)
        ]
    )
    derivative = np.zeros((4, 4))
    for target in range(4):
        for source in range(4):
            if target != source:
                derivative[target, source] = (
                    barycentric[source] / barycentric[target] / (points[target] - points[source])
                )
    legendre = np.stack(
        [np.ones(4), points, (3.0 * points**2 - 1.0) / 2.0, (5.0 * points**3 - 3.0 * points) / 2.0],
        1,
    )
    legendre = legendre * np.sqrt(np.arange(4) + 0.5)
    weight_column = np.array(weights)[:, None]
    discrete_norms = np.sum(weight_column * legendre * legendre, 0)
    inverse = (weight_column * legendre).T / discrete_norms[:, None]
    return (weights, derivative, inverse)


def mechanics(conserved):
    density, m1, m2, m3, energy = conserved
    inverse = 1.0 / density
    v1, v2, v3 = m1 * inverse, m2 * inverse, m3 * inverse
    pressure = (gas_gamma - 1.0) * (energy - 0.5 * density * (v1 * v1 + v2 * v2 + v3 * v3))
    sound = jnp.sqrt(gas_gamma * pressure * inverse)
    return [v1, v2, v3, pressure, sound]


def logarithms(density, pressure):
    ratio = density / pressure
    return [jnp.log(density), jnp.log(ratio), ratio]


def primitives(conserved):
    motion = mechanics(conserved)
    return list(conserved) + motion + logarithms(conserved[0], motion[3])


def mean_parts(a, b, log_a, log_b):
    total, gap = a + b, a - b
    relative = gap / total
    square = relative * relative
    small = square < 0.01
    series = 2.0 + square * (2.0 / 3.0 + square * (2.0 / 5.0 + square * (2.0 / 7.0)))
    return jnp.where(small, total, gap), jnp.where(small, series, log_a - log_b)


def entropy_flux(a, b, normal):
    num, den = mean_parts(a[0], b[0], a[LND], b[LND])
    mean_density = num / den
    num, den = mean_parts(a[RAT], b[RAT], a[LNR], b[LNR])
    inverse_beta = den / num
    velocity = [0.5 * (a[VEL + i] + b[VEL + i]) for i in range(3)]
    pressure = 0.5 * (a[PRS] + b[PRS])
    product = 0.5 * (a[5] * b[5] + a[6] * b[6] + a[7] * b[7])
    mass = mean_density * velocity[normal]
    out = [mass]
    for other in range(3):
        momentum = mass * velocity[other]
        out.append(momentum + pressure if other == normal else momentum)
    out.append(
        mass * (product + inverse_beta * (1.0 / (gas_gamma - 1.0)))
        + 0.5 * (a[PRS] * b[VEL + normal] + b[PRS] * a[VEL + normal])
    )
    return out


def dissipated(flux, a, b, normal):
    half = 0.5 * jnp.maximum(
        jnp.abs(a[VEL + normal]) + a[SND], jnp.abs(b[VEL + normal]) + b[SND]
    )
    return [flux[i] - half * (b[i] - a[i]) for i in range(5)]


def line_terms(nodes, normal, weights, deriv):
    vol = [[0.0] * 5 for _ in range(4)]
    diff = [[0.0] * 5 for _ in range(4)]
    for i in range(4):
        for j in range(i + 1, 4):
            flux = entropy_flux(nodes[i], nodes[j], normal)
            ci, cj = 2.0 * float(deriv[i, j]), 2.0 * float(deriv[j, i])
            if j == i + 1:
                face = dissipated(flux, nodes[i], nodes[j], normal)
            for f in range(5):
                vi, vj = ci * flux[f], cj * flux[f]
                vol[i][f] = vol[i][f] + vi
                vol[j][f] = vol[j][f] + vj
                if j == i + 1:
                    diff[i][f] = diff[i][f] + (face[f] * (1.0 / weights[i]) - vi)
                    diff[j][f] = diff[j][f] - (face[f] * (1.0 / weights[j]) + vj)
                else:
                    diff[i][f] = diff[i][f] - vi
                    diff[j][f] = diff[j][f] - vj
    return vol, diff


def make_kernel(ngx, ngy, nx, ny, nz):
    weights, deriv, inverse = tables()
    exl, eyl, rows = nx // 4, ny // 4, nx * ny
    total = ngx * ngy
    parts = 10 * (nx + ny) + 4 * exl * eyl
    roots = [(0, 0), (ngx - 1, 0), (1, 1), (1, 0)]
    group = 8 if (nx * eyl) % 8 == 0 else 4

    def kernel(u_in, inc, smooth_out, top_out, st, vol, dif, tq, ysend, yrecv, xrecv, yown, rb, rbr, near,
               bsc, mx, mx2, mxr, myr, span, sent, halo, tops, late):
        ix, iy = lax.axis_index("gx"), lax.axis_index("gy")
        loads = [pltpu.make_async_copy(u_in.at[f], st.at[f, BASE:BASE + rows], sent) for f in range(5)]
        for c in loads:
            c.start()
        barrier = pltpu.get_barrier_semaphore()
        rank = iy * ngx + ix
        is_root = [rank == y * ngx + x for x, y in roots]
        root = is_root[0]
        for here in is_root[1:]:
            root = jnp.logical_or(root, here)

        def greet(device):
            pl.semaphore_signal(barrier, 1, device_id=device, device_id_type=MESH)

        def visit(act):
            def step(k, carry):
                t = k + jnp.where(k >= rank, 1, 0)
                act({"gx": lax.rem(t, ngx), "gy": lax.div(t, ngx)})
                return carry

            lax.fori_loop(0, total - 1, step, 0)

        xup, xdn = {"gx": lax.rem(ix + 1, ngx)}, {"gx": lax.rem(ix + ngx - 1, ngx)}
        yup, ydn = {"gy": lax.rem(iy + 1, ngy)}, {"gy": lax.rem(iy + ngy - 1, ngy)}
        inner, wraps = iy > 0, iy == ngy - 1
        need = jnp.where(root, 6, 7) + jnp.where(inner, 1, 0)
        for device in (xup, xdn, ydn):
            greet(device)
        pl.when(jnp.logical_not(wraps))(lambda: greet(yup))

        @pl.when(root)
        def _():
            visit(greet)


        def remote(src, dst, rs, dev):
            return pltpu.make_async_remote_copy(
                src_ref=src, dst_ref=dst, send_sem=sent, recv_sem=rs, device_id=dev,
                device_id_type=MESH)

        def all_of(ref, count, sem):
            return remote(ref.at[0:count], ref.at[0:count], sem, xup)

        pltpu.make_async_copy(u_in, st.at[0:5, BASE:BASE + rows], sent).wait()
        top = None
        for r in range(0, rows, 8):
            density, m1, m2, m3, energy = [st[f, BASE + r:BASE + r + 8, :] for f in range(5)]
            unit = 1.0 / density
            v1, v2, v3 = m1 * unit, m2 * unit, m3 * unit
            inside = energy - 0.5 * density * (v1 * v1 + v2 * v2 + v3 * v3)
            sound = jnp.sqrt(gas_gamma * (gas_gamma - 1.0) * inside * unit)
            speed = jnp.abs(v1) + jnp.abs(v2) + jnp.abs(v3) + 3.0 * sound
            top = speed if top is None else jnp.maximum(top, speed)
        mx[...] = jnp.max(top, axis=0, keepdims=True)
        last = jnp.logical_and(wraps, ix >= ngx - 2)

        def meet():
            pl.semaphore_wait(barrier, need)

            for (x, y), here in zip(roots, is_root):
                @pl.when(jnp.logical_not(here))
                def _():
                    remote(mx, mxr.at[pl.ds(rank, 1)], tops, {"gx": x, "gy": y}).start()

        pl.when(last)(meet)
        lane = lax.broadcasted_iota(jnp.int32, (8, nz), 1)
        k = lane % 4
        k0, k1, k2, k3 = k == 0, k == 1, k == 2, k == 3

        def lanes(values):
            a, b, c, d = (float(v) for v in values)
            return jnp.where(k0, a, jnp.where(k1, b, jnp.where(k2, c, d))).astype(jnp.float32)

        def roll(x, s):
            return pltpu.roll(x, s % nz, 1)

        zcoef = {s: lanes([inverse[c, c + s] if 0 <= c + s < 4 else 0.0 for c in range(4)])
                 for s in range(-3, 4)}
        for r in range(0, rows, 8):
            here = slice(BASE + r, BASE + r + 8)
            p = mechanics([st[f, here, :] for f in range(5)])
            for f in range(5):
                st[VEL + f, here, :] = p[f]
            q = st[0, here, :] * p[3]
            t = zcoef[0] * q
            for s in (-3, -2, -1, 1, 2, 3):
                t = t + zcoef[s] * roll(q, -s)
            tq[r:r + 8, :] = t

        ke = k[:eyl]
        for e in range(exl):
            nodes = [[tq[pl.ds((4 * e + i) * ny + j, eyl, 4), :] for j in range(4)]
                     for i in range(4)]
            half = [[sum(float(inverse[a, i]) * nodes[i][j] for i in range(4))
                     for j in range(4)] for a in range(4)]
            e2 = e3 = e4 = 0.0
            for a in range(4):
                for b in range(4):
                    m = sum(float(inverse[b, j]) * half[a][j] for j in range(4))
                    m = m * m
                    e4 = e4 + m
                    if a < 3 and b < 3:
                        e3 = e3 + m
                    if a < 2 and b < 2:
                        e2 = e2 + m
            e3 = jnp.where(ke < 3, e3, 0.0)
            e2 = jnp.where(ke < 2, e2, 0.0)

            def spread(x):
                total = x
                for s in range(1, 4):
                    total = total + jnp.where(ke + s < 4, roll(x, -s), roll(x, 4 - s))
                return total

            e2, e3, e4 = spread(e2), spread(e3), spread(e4)
            energy = jnp.maximum((e4 - e3) / (e4 + 1e-06), (e3 - e2) / (e3 + 1e-06))
            threshold = 0.5 * 10.0 ** (-1.8 * 4.0**0.25)
            sharp = math.log(9999.0) / threshold
            raw = 1.0 / (1.0 + jnp.exp(-sharp * (energy - threshold)))
            raw = jnp.minimum(raw, 0.5)
            rb[e] = raw
        for f in range(5):
            ysend[0, f] = st[f, pl.ds(BASE + ny - 1, nx, ny), :]
            ysend[1, f] = st[f, pl.ds(BASE, nx, ny), :]
        mxr[pl.ds(rank, 1), :] = mx[...]

        pl.when(jnp.logical_not(last))(meet)
        remote(ysend.at[0], yrecv.at[0], halo, yup).start()
        pl.when(inner)(lambda: remote(ysend.at[1], yrecv.at[1], halo, ydn).start())
        remote(st.at[0:5, BASE + rows - ny:BASE + rows], xrecv.at[0], halo, xup).start()
        remote(st.at[0:5, BASE:BASE + ny], xrecv.at[1], halo, xdn).start()
        remote(rb, rbr.at[2], halo, yup).start()
        pl.when(inner)(lambda: remote(rb, rbr.at[3], halo, ydn).start())
        remote(rb, rbr.at[0], halo, xup).start()
        remote(rb, rbr.at[1], halo, xdn).start()

        @pl.when(wraps)
        def _():
            pl.semaphore_signal(late, 1, device_id=yup, device_id_type=MESH)

        for r in range(0, rows, 8):
            here = slice(BASE + r, BASE + r + 8)
            p = logarithms(st[0, here, :], st[PRS, here, :])
            for f in range(3):
                st[LND + f, here, :] = p[f]
        for e in range(exl):
            raw = rb[e]
            close = jnp.maximum(roll(raw, 4), roll(raw, -4))
            if e > 0:
                close = jnp.maximum(close, rb[e - 1])
            if e < exl - 1:
                close = jnp.maximum(close, rb[e + 1])
            near[e, 8:8 + eyl, :] = raw
            near[e, 7:8, :] = raw[0:1]
            near[e, 8 + eyl:9 + eyl, :] = raw[eyl - 1:eyl]
            close = jnp.maximum(close, jnp.maximum(near[e, 7:7 + eyl, :], near[e, 9:9 + eyl, :]))
            bsc[e] = close

        ca = lanes([2 * deriv[0, 1], 2 * deriv[1, 2], 2 * deriv[2, 3], 1 / weights[3]])
        cb = lanes([2 * deriv[1, 0], 2 * deriv[2, 1], 2 * deriv[3, 2], -1 / weights[0]])
        da = lanes([1 / weights[0], 1 / weights[1], 1 / weights[2], 0.0])
        db = lanes([-1 / weights[1], -1 / weights[2], -1 / weights[3], 0.0])
        cam = jnp.where(k3, 0.0, ca)
        cbm = jnp.where(k3, 0.0, cb)
        mc = lanes([2 * deriv[0, 2], 2 * deriv[1, 3], 0.0, 2 * deriv[3, 0]])
        mr_ = lanes([2 * deriv[0, 3], 0.0, 2 * deriv[2, 0], 2 * deriv[3, 1]])

        def z_group(g, carry):
            row = pl.multiple_of(g * 8, 8)
            own = [st[f, pl.ds(row + BASE, 8), :] for f in range(FIELDS)]
            nxt = [roll(x, -1) for x in own]
            far = [None] * FIELDS
            for f in (0, 5, 6, 7, PRS, LND, LNR, RAT):
                far[f] = jnp.where(k < 2, roll(own[f], -2), roll(own[f], 3))
            f1 = entropy_flux(own, nxt, 2)
            g1 = dissipated(f1, own, nxt, 2)
            fm = entropy_flux(own, far, 2)
            for f in range(5):
                sel = jnp.where(k3, g1[f], f1[f])
                mm = mc * fm[f] + mr_ * jnp.where(k0, roll(fm[f], -3), roll(fm[f], 2))
                vol[f, pl.ds(row, 8), :] = ca * sel + roll(cb * sel, 1) + mm
                dif[f, pl.ds(row, 8), :] = (
                    (da * g1[f] - cam * f1[f]) + roll(db * g1[f] - cbm * f1[f], 1) - mm)
            return carry

        lax.fori_loop(0, rows // 8, z_group, 0)

        for e in range(exl):
            for h in range(0, ny, 8):
                slabs = [(4 * e + i) * ny + h for i in range(4)]
                nodes = [[st[f, BASE + r:BASE + r + 8, :] for f in range(FIELDS)] for r in slabs]
                va, da_ = line_terms(nodes, 0, weights, deriv)
                for i in range(4):
                    for f in range(5):
                        vol[f, slabs[i]:slabs[i] + 8, :] += va[i][f]
                        dif[f, slabs[i]:slabs[i] + 8, :] += da_[i][f]
        for g in range(0, nx * eyl, group):
            def rows_of(ref, f, i, base):
                return ref[f, pl.ds(base + 4 * g + i, group, 4), :]

            nodes = [[rows_of(st, f, i, BASE) for f in range(FIELDS)] for i in range(4)]
            va, da_ = line_terms(nodes, 1, weights, deriv)
            for i in range(4):
                for f in range(5):
                    vol[f, pl.ds(4 * g + i, group, 4), :] += va[i][f]
                    dif[f, pl.ds(4 * g + i, group, 4), :] += da_[i][f]

        for e in range(1, exl):
            for h in range(0, ny, 8):
                r = 4 * e * ny + h
                a = [st[f, BASE + r - ny:BASE + r - ny + 8, :] for f in range(FIELDS)]
                b = [st[f, BASE + r:BASE + r + 8, :] for f in range(FIELDS)]
                face = dissipated(entropy_flux(a, b, 0), a, b, 0)
                for f in range(5):
                    vol[f, r - ny:r - ny + 8, :] += face[f] * (1.0 / weights[3])
                    vol[f, r:r + 8, :] -= face[f] * (1.0 / weights[0])
        for g in range(0, nx * eyl, group):
            ye = (lax.broadcasted_iota(jnp.int32, (group, nz), 0) + g) % eyl
            inside = ye < eyl - 1
            a = [st[f, pl.ds(BASE + 4 * g + 3, group, 4), :] for f in range(FIELDS)]
            b = [st[f, pl.ds(BASE + 4 * g + 4, group, 4), :] for f in range(FIELDS)]
            face = dissipated(entropy_flux(a, b, 1), a, b, 1)
            for f in range(5):
                kept = jnp.where(inside, face[f], 0.0)
                vol[f, pl.ds(4 * g + 3, group, 4), :] += kept * (1.0 / weights[3])
                vol[f, pl.ds(4 * g + 4, group, 4), :] -= kept * (1.0 / weights[0])
        for f in range(FIELDS):
            yown[f, 0:nx] = st[f, pl.ds(BASE, nx, ny), :]
            yown[f, nx:2 * nx] = st[f, pl.ds(BASE + ny - 1, nx, ny), :]

        @pl.when(jnp.logical_not(inner))
        def _():
            pl.semaphore_wait(late, 1)
            remote(ysend.at[1], yrecv.at[1], halo, ydn).start()
            remote(rb, rbr.at[3], halo, ydn).start()

        all_of(span, parts, halo).wait_recv()
        for h in range(0, ny, 8):
            for side in range(2):
                got = primitives([xrecv[side, f, h:h + 8, :] for f in range(5)])
                r = h if side == 0 else rows - ny + h
                own = [st[f, BASE + r:BASE + r + 8, :] for f in range(FIELDS)]
                a, b = (got, own) if side == 0 else (own, got)
                face = dissipated(entropy_flux(a, b, 0), a, b, 0)
                scale = -1.0 / weights[0] if side == 0 else 1.0 / weights[3]
                for f in range(5):
                    vol[f, r:r + 8, :] += face[f] * scale

        row = lax.broadcasted_iota(jnp.int32, (eyl, nz), 0)
        pick = (lax.broadcasted_iota(jnp.int32, (nz, nz // 4), 0)
                == 4 * lax.broadcasted_iota(jnp.int32, (nz, nz // 4), 1)).astype(jnp.float32)
        for e in range(exl):
            close = bsc[e]
            if e == 0:
                close = jnp.maximum(close, rbr[0, exl - 1])
            if e == exl - 1:
                close = jnp.maximum(close, rbr[1, 0])
            close = jnp.maximum(close, jnp.where(row == 0, rbr[2, e, eyl - 1:eyl, :], 0.0))
            close = jnp.maximum(close, jnp.where(row == eyl - 1, rbr[3, e, 0:1, :], 0.0))
            smooth = jnp.maximum(rb[e], 0.5 * close)
            bsc[e] = smooth
            smooth_out[e] = jnp.dot(smooth, pick, precision=lax.Precision.HIGHEST,
                                    preferred_element_type=jnp.float32)

        got = primitives([jnp.concatenate([yrecv[0, f], yrecv[1, f]], axis=0) for f in range(5)])
        own = [yown[f] for f in range(FIELDS)]
        first = lax.broadcasted_iota(jnp.int32, (2 * nx, nz), 0) < nx
        a = [jnp.where(first, got[f], own[f]) for f in range(FIELDS)]
        b = [jnp.where(first, own[f], got[f]) for f in range(FIELDS)]
        face = dissipated(entropy_flux(a, b, 1), a, b, 1)
        for f in range(5):
            vol[f, pl.ds(0, nx, ny), :] -= face[f][:nx] * (1.0 / weights[0])
            vol[f, pl.ds(ny - 1, nx, ny), :] += face[f][nx:] * (1.0 / weights[3])
        under = lax.broadcasted_iota(jnp.int32, (8, nz), 0) < 4
        for e in range(exl):
            for h in range(0, ny, 8):
                y = h // 4
                b = jnp.where(under, bsc[e, y:y + 1, :], bsc[e, y + 1:y + 2, :])
                for i in range(4):
                    r = (4 * e + i) * ny + h
                    for f in range(5):
                        inc[f, r:r + 8, :] = vol[f, r:r + 8, :] + b * dif[f, r:r + 8, :]
        for here, count in ((root, 3), (jnp.logical_not(root), 4)):
            @pl.when(here)
            def _():
                all_of(span, parts + count, tops).wait_send()

        def gather():
            all_of(span, total - 1, tops).wait_recv()
            found = [mxr[i:i + 8, :] for i in range(0, total, 8)]
            while len(found) > 1:
                pairs = [jnp.maximum(a, b) for a, b in zip(found[::2], found[1::2])]
                found = pairs + found[2 * len(pairs):]
            return jnp.max(found[0], axis=0, keepdims=True)

        for hub, mine in ((1, lambda x, odd: x >= 2 or not odd), (2, lambda x, odd: x < 2 and odd)):
            @pl.when(is_root[hub])
            def _():
                mx2[...] = gather()

                def send(h, carry):
                    for odd in range(2):
                        for x in range(ngx):
                            if mine(x, odd) and not (isinstance(h, int) and (x, 2 * h + odd) in roots):
                                remote(mx2, myr, tops, {"gx": x, "gy": 2 * h + odd}).start()
                    return carry

                for h in range(min(ngy // 2, 16)):
                    send(h, 0)
                if ngy > 32:
                    lax.fori_loop(16, ngy // 2, send, 0)
                top_out[...] = mx2[...]
                count = sum(mine(x, y % 2) and (x, y) not in roots
                            for x in range(ngx) for y in range(ngy))
                all_of(span, count, tops).wait_send()

        @pl.when(jnp.logical_not(root))
        def _():
            remote(mx2, myr, tops, xup).wait_recv()
            top_out[...] = myr[...]

        @pl.when(jnp.logical_or(is_root[0], is_root[3]))
        def _():
            top_out[...] = gather()

    f32 = jnp.float32
    dma = pltpu.SemaphoreType.DMA
    pad = BASE + rows + 8
    scratch = [
        pltpu.VMEM((FIELDS, pad, nz), f32),
        pltpu.VMEM((5, rows + 8, nz), f32),
        pltpu.VMEM((5, rows, nz), f32),
        pltpu.VMEM((rows, nz), f32),
        pltpu.VMEM((2, 5, nx, nz), f32),
        pltpu.VMEM((2, 5, nx, nz), f32),
        pltpu.VMEM((2, 5, ny, nz), f32),
        pltpu.VMEM((FIELDS, 2 * nx, nz), f32),
        pltpu.VMEM((exl, eyl, nz), f32),
        pltpu.VMEM((4, exl, eyl, nz), f32),
        pltpu.VMEM((exl, eyl + 16, nz), f32),
        pltpu.VMEM((exl, eyl, nz), f32),
        pltpu.VMEM((1, nz), f32),
        pltpu.VMEM((1, nz), f32),
        pltpu.VMEM((total, nz), f32),
        pltpu.VMEM((1, nz), f32),
        pltpu.VMEM((max(parts + 4, total), 1, nz), f32),
        dma, dma, dma,
        pltpu.SemaphoreType.REGULAR,
    ]
    return kernel, scratch


def finish(raw, smooth, top, inc, bl, scaled, done):
    blend = pltpu.make_async_copy(smooth, bl, done)
    blend.start()
    peak = jnp.broadcast_to(top[...], (8, top.shape[1]))
    step = -0.25 / jnp.max(peak, axis=1, keepdims=True)
    rows = raw.shape[1]
    half = max(rows // 16 * 8, 8)
    for f in range(5):
        for low in range(0, rows, half):
            high = min(low + half, rows)
            for r in range(low, high, 8):
                scaled[f, r:r + 8, :] = step * raw[f, r:r + 8, :]
            pltpu.make_async_copy(scaled.at[f, low:high], inc.at[f, low:high], done).start()
    pltpu.make_async_copy(scaled, inc, done).wait()
    blend.wait()


def solution(mesh):
    ngx, ngy = mesh.shape["gx"], mesh.shape["gy"]

    def body(conserved):
        _, nx, ny, nz = conserved.shape
        kernel, scratch = make_kernel(ngx, ngy, nx, ny, nz)
        vmem = pl.BlockSpec(memory_space=pltpu.VMEM)
        shape = lambda *dims: jax.ShapeDtypeStruct(dims, jnp.float32)
        raw, smooth, top = pl.pallas_call(
            kernel,
            out_shape=(shape(5, nx * ny, nz), shape(nx // 4, ny // 4, nz // 4), shape(1, nz)),
            in_specs=[pl.BlockSpec(memory_space=pltpu.HBM)],
            out_specs=(vmem, vmem, vmem),
            scratch_shapes=scratch,
            compiler_params=pltpu.CompilerParams(
                collective_id=0, has_side_effects=True, vmem_limit_bytes=12 * 2**20),
            name="section",
        )(pltpu.with_memory_space_constraint(
            conserved.reshape(5, nx * ny, nz), pltpu.HBM))
        inc, blending = pl.pallas_call(
            finish,
            out_shape=(shape(5, nx * ny, nz), shape(nx // 4, ny // 4, nz // 4)),
            in_specs=[vmem, vmem, vmem],
            out_specs=(pl.BlockSpec(memory_space=pltpu.HBM),) * 2,
            scratch_shapes=[pltpu.VMEM((5, nx * ny, nz), jnp.float32), pltpu.SemaphoreType.DMA],
            compiler_params=pltpu.CompilerParams(vmem_limit_bytes=8 * 2**20),
            name="finish",
        )(raw, smooth, top)
        return inc.reshape(conserved.shape), blending

    return jax.shard_map(
        body, mesh=mesh, in_specs=(P(None, "gx", "gy", None),),
        out_specs=(P(None, "gx", "gy", None), P("gx", "gy", None)), check_vma=False)
```
